128 devices in a mesh: tm: 16 (over z, y), space: 8 (over x, core).
Axes of the slice: x: 4, y: 4, z: 4, core: 2. Of those that a mesh axis runs over, the one named last changes fastest.
Arguments:
- attn_query: bfloat16 [16384, 2560], P(('tm', 'space')), may hold values from -8 to 8
- attn_key: bfloat16 [16384, 2560], P(('tm', 'space')), may hold values from -8 to 8
- attn_value: bfloat16 [16384, 2560], P(('tm', 'space')), may hold values from -6 to 6
- attn_outgrad: bfloat16 [16384, 2560], P(('tm', 'space')), may hold values from -6 to 6
- fast_query: bfloat16 [16384, 1536], P('tm'), may hold values from -6 to 6
- fast_outgrad: bfloat16 [16384, 1536], P('tm'), may hold values from -6 to 6
- fast_key: bfloat16 [16384, 1536], P('tm'), may hold values from -6 to 6
- gate_weights: bfloat16 [16, 1536, 3072], P('tm', None, 'space'), may hold values from -0.15625 to 0.15625
- up_weights: bfloat16 [16, 1536, 3072], P('tm', None, 'space'), may hold values from -0.15625 to 0.15625
- down_weights: bfloat16 [16, 3072, 1536], P('tm', 'space'), may hold values from -0.109375 to 0.109375
- gate_factor: bfloat16 [16384, 3072], P('tm', 'space'), may hold values from -0.15625 to 0.15625
- clip_groups: int32 [4], replicated, may hold values from 1 to 8, 16 in all
Outputs:
- query_grad: bfloat16 [16384, 2560], P(('tm', 'space'))
- key_grad: bfloat16 [16384, 2560], P(('tm', 'space'))
- value_grad: bfloat16 [16384, 2560], P(('tm', 'space'))
- fast_grad: bfloat16 [16384, 1536], P(('tm', 'space'))
- rate_grad: float32 [16384], P(('tm', 'space'))
The draws below stay inside these ranges and needn't reach their ends.
Inputs may be any that keep to these rules, and one draw needn't show every extreme that they name: `clip_groups`: clip k covers the groups after those of clips 0 to k - 1; the counts sum to 16.
All inputs are finite; a program needn't handle non-finite values.
Results may differ from the reference program's by a relative error of at most 0.012.
Values may be sent and summed in bfloat16 or wider, within the bound.
A program may use at most 192 MiB of HBM per device.

```python
import math
import jax
import jax.numpy as jnp
import numpy as np
from jax import lax

HEAD = 128
FD = 1536
FH = 3072
NCLIPS = 4
TILE = 128
D = 2560
REACH = 64
ROWS = 1024
GROUPS = 16
TOTAL = 16384
MOST = 8
N_SPACE = 8


def paired_rows(key):
    base = jax.random.fold_in(key, 7)
    first_key, second_key = jax.random.split(base, 2)
    queries = jnp.clip(jax.random.normal(first_key, (TOTAL, D), jnp.float32), -6.0, 6.0)
    keys_drawn = jnp.clip(jax.random.normal(second_key, (TOTAL, D), jnp.float32), -6.0, 6.0)
    return (queries, keys_drawn)


def draw_attn_query(key, part):
    return paired_rows(key)[0].astype(jnp.bfloat16)


def draw_attn_key(key, part):
    return paired_rows(key)[1].astype(jnp.bfloat16)


def steps_of(own_key, extent, cuts, smallest, high):
    level = 1.0
    for dim, parts in cuts:
        heights = jax.random.uniform(jax.random.fold_in(jax.random.fold_in(own_key, 6), dim), (parts,), jnp.float32, smallest / len(cuts), high / len(cuts))
        level = level * jnp.repeat(jnp.exp(heights), extent[dim] // parts).reshape((-1,) + (1,) * (len(extent) - 1 - dim))
    return level


def split_up(number_of, total, reach, skew):
    weights = [(1 << 20) // math.isqrt(rank ** skew) + 1 for rank in range(2, number_of + 1)]
    rest, holding = total - reach - (number_of - 1), [1] * (number_of - 1)
    while rest > 0:
        movable = [i for i in range(number_of - 1) if holding[i] < reach]
        mass, budget = sum([weights[i] for i in movable]), rest
        for i in movable:
            extra = min(reach - holding[i], max(1, budget * weights[i] // mass), rest)
            holding[i] = holding[i] + extra
            rest = rest - extra
    return np.array([reach] + holding)


def ragged(stream_key, amount, total, reach, lean):
    if amount == 2:
        one = jax.random.randint(stream_key, (), max(1, total - reach), min(reach, total - 1) + 1)
        return jnp.stack([one, total - one])
    sizes = jnp.asarray(split_up(amount, total, reach, lean), jnp.int32)
    twos = (amount - 1) // 2
    source_of, sink = sizes[1:1 + 2 * twos:2], sizes[2:2 + 2 * twos:2]
    slack = jnp.minimum(source_of - 1, reach - sink)
    passed = jax.random.randint(jax.random.fold_in(stream_key, 1), (twos,), 0, 1 << 20) % (slack + 1)
    sizes = sizes.at[1:1 + 2 * twos:2].set(source_of - passed).at[2:2 + 2 * twos:2].set(sink + passed)
    return sizes[jax.random.permutation(jax.random.fold_in(stream_key, 2), amount)]


def scatter_about(own_key, extent, scale, reach, shards=(), held_as=jnp.bfloat16):
    factor_of = steps_of(own_key, extent, shards, -0.22, 0.18) if shards else 1.0
    entries = jax.random.normal(own_key, extent, jnp.float32) * scale * factor_of
    return jnp.minimum(jnp.maximum(entries, -reach), reach).astype(held_as)


def setup_inputs(seed: int = 0) -> dict:
    splits = jax.random.split(jax.random.key(seed), 13)
    return {
        "attn_query": draw_attn_query(jax.random.fold_in(splits[12], 71), 0),
        "attn_key": draw_attn_key(jax.random.fold_in(splits[12], 71), 0),
        "attn_value": scatter_about(splits[2], (TOTAL, D), 1.0, 6.0, ((0, 128),)),
        "attn_outgrad": scatter_about(splits[3], (TOTAL, D), 1.0, 6.0, ((0, 128),)),
        "fast_query": scatter_about(splits[4], (TOTAL, FD), 1.0, 6.0, ((0, 16),)),
        "fast_outgrad": scatter_about(splits[5], (TOTAL, FD), 1.0, 6.0, ((0, 16),)),
        "fast_key": scatter_about(splits[6], (TOTAL, FD), 1.0, 6.0, ((0, 16),)),
        "gate_weights": scatter_about(splits[7], (GROUPS, FD, FH), FD ** -0.5, 0.15625, ((0, 16), (2, 8))),
        "up_weights": scatter_about(splits[8], (GROUPS, FD, FH), FD ** -0.5, 0.15625, ((0, 16), (2, 8))),
        "down_weights": scatter_about(splits[9], (GROUPS, FH, FD), FH ** -0.5, 0.109375, ((0, 16), (1, 8))),
        "gate_factor": scatter_about(splits[10], (TOTAL, FH), FD ** -0.5, 0.15625, ((0, 16), (1, 8))),
        "clip_groups": ragged(splits[11], NCLIPS, GROUPS, MOST, 2).astype(jnp.int32),
    }


def window_grads(queries, key_rows, value_rows, out_grad, query_pos, key_pos, key_live):
    head_count = queries.shape[1] // HEAD
    query_heads = queries.astype(jnp.float32).reshape(queries.shape[0], head_count, HEAD)
    key_heads = key_rows.astype(jnp.float32).reshape(key_rows.shape[0], head_count, HEAD)
    value_heads = value_rows.astype(jnp.float32).reshape(value_rows.shape[0], head_count, HEAD)
    grad_heads = out_grad.astype(jnp.float32).reshape(out_grad.shape[0], head_count, HEAD)
    scaling = 1.0 / math.sqrt(HEAD)
    scores = jnp.einsum('qhd,khd->hqk', query_heads, key_heads) * scaling
    allowed = key_live[None, :] & (jnp.abs(query_pos[:, None] - key_pos[None, :]) <= REACH)
    scores = jnp.where(allowed[None], scores, -1e+30)
    peak_score = lax.optimization_barrier(jnp.max(scores, axis=2, keepdims=True))
    exponent = jnp.exp(scores - peak_score)
    attn_weights = exponent / lax.optimization_barrier(jnp.sum(exponent, axis=2, keepdims=True))
    weights_b = lax.optimization_barrier(attn_weights.astype(jnp.bfloat16)).astype(jnp.float32)
    attn_out = jnp.einsum('hqk,khd->qhd', weights_b, value_heads)
    row_delta = lax.optimization_barrier(jnp.sum(grad_heads * attn_out, axis=2))
    value_grad = jnp.einsum('hqk,qhd->khd', weights_b, grad_heads)
    weight_grad = jnp.einsum('qhd,khd->hqk', grad_heads, value_heads)
    score_grad = attn_weights * (weight_grad - jnp.transpose(row_delta)[:, :, None])
    score_grad_b = lax.optimization_barrier(score_grad.astype(jnp.bfloat16)).astype(jnp.float32)
    query_grad = jnp.einsum('hqk,khd->qhd', score_grad_b, key_heads) * scaling
    key_grad = jnp.einsum('hqk,qhd->khd', score_grad_b, query_heads) * scaling
    return (query_grad.reshape(queries.shape[0], -1), key_grad.reshape(key_rows.shape[0], -1), value_grad.reshape(value_rows.shape[0], -1))

def assemble(extended):
    blocks = extended.reshape(GROUPS, N_SPACE, TILE + 2 * REACH, D)
    middle = blocks[:, :, REACH:REACH + TILE]
    from_left = jnp.pad(blocks[:, :-1, TILE + REACH:], ((0, 0), (1, 0), (0, TILE - REACH), (0, 0)))
    from_right = jnp.pad(blocks[:, 1:, :REACH], ((0, 0), (0, 1), (TILE - REACH, 0), (0, 0)))
    return (middle + from_left + from_right).reshape(TOTAL, D).astype(jnp.bfloat16)

def reference(attn_query, attn_key, attn_value, attn_outgrad, fast_query, fast_outgrad, fast_key, gate_weights, up_weights, down_weights, gate_factor, clip_groups):
    tile_count = GROUPS * N_SPACE
    query_tiles = attn_query.reshape(tile_count, TILE, D)
    grad_tiles = attn_outgrad.reshape(tile_count, TILE, D)
    key_pad = jnp.pad(attn_key.reshape(GROUPS, ROWS, D), ((0, 0), (REACH, REACH), (0, 0)))
    value_pad = jnp.pad(attn_value.reshape(GROUPS, ROWS, D), ((0, 0), (REACH, REACH), (0, 0)))

    def per_tile(inputs):
        queries, out_grad, index = inputs
        group = index // N_SPACE
        start = (index % N_SPACE * TILE).astype(jnp.int32)
        key_rows = lax.dynamic_slice_in_dim(lax.dynamic_index_in_dim(key_pad, group, 0, False), start, TILE + 2 * REACH, 0)
        value_rows = lax.dynamic_slice_in_dim(lax.dynamic_index_in_dim(value_pad, group, 0, False), start, TILE + 2 * REACH, 0)
        query_pos = start + jnp.arange(TILE, dtype=jnp.int32)
        key_pos = start - REACH + jnp.arange(TILE + 2 * REACH, dtype=jnp.int32)
        key_live = (key_pos >= 0) & (key_pos < ROWS)
        return window_grads(queries, key_rows, value_rows, out_grad, query_pos, key_pos, key_live)
    query_all, key_ext, value_ext = lax.map(per_tile, (query_tiles, grad_tiles, jnp.arange(tile_count, dtype=jnp.int32)))
    query_grad = query_all.reshape(TOTAL, D).astype(jnp.bfloat16)
    key_grad = assemble(key_ext)
    value_grad = assemble(value_ext)
    starts = jnp.cumsum(clip_groups) - clip_groups
    first = jnp.any(starts[None, :] == jnp.arange(GROUPS, dtype=jnp.int32)[:, None], axis=1).astype(jnp.float32)
    contract_rows = (((0,), (0,)), ((), ()))
    contract_last = (((1,), (1,)), ((), ()))

    def backward_step(gate_carry, inputs):
        queries, out_grad, key_rows, gate_w, up_w, down_w, gate_f, flag = inputs
        gate_pre = jnp.dot(queries, gate_w, preferred_element_type=jnp.float32)
        up_pre = jnp.dot(queries, up_w, preferred_element_type=jnp.float32)
        gate_sig = jax.nn.sigmoid(gate_pre)
        gate_act = gate_pre * gate_sig
        hidden_grad = lax.dot_general(out_grad, down_w, contract_last, preferred_element_type=jnp.float32)
        gate_grad_b = (hidden_grad * up_pre * gate_sig * (1.0 + gate_pre * (1.0 - gate_sig))).astype(jnp.bfloat16)
        up_grad_b = (hidden_grad * gate_act).astype(jnp.bfloat16)
        input_grad = lax.dot_general(gate_grad_b, gate_w, contract_last, preferred_element_type=jnp.float32) + lax.dot_general(up_grad_b, up_w, contract_last, preferred_element_type=jnp.float32)
        rate = lax.optimization_barrier(jnp.sum(jnp.dot(key_rows, gate_carry.astype(jnp.bfloat16), preferred_element_type=jnp.float32) * gate_f, axis=1)) / ROWS
        gate_total = lax.dot_general(queries, gate_grad_b, contract_rows, preferred_element_type=jnp.float32)
        renewed = (1.0 - flag) * (gate_carry + gate_total)
        return (renewed, (input_grad.astype(jnp.bfloat16), rate))
    initial = jnp.zeros((FD, FH), jnp.float32)
    inputs = (fast_query.reshape(GROUPS, ROWS, FD), fast_outgrad.reshape(GROUPS, ROWS, FD), fast_key.reshape(GROUPS, ROWS, FD), gate_weights, up_weights, down_weights, gate_factor.reshape(GROUPS, ROWS, FH), first)
    ending, outputs = lax.scan(backward_step, initial, inputs, reverse=True)
    fast_grad = outputs[0].reshape(TOTAL, FD)
    rate_grad = outputs[1].reshape(TOTAL)
    return (query_grad, key_grad, value_grad, fast_grad, rate_grad)
```

```python
import functools
import math

import jax
import jax.numpy as jnp
from jax import lax
from jax.experimental import pallas as pl
from jax.experimental.pallas import tpu as pltpu
from jax.sharding import PartitionSpec as P

MESH = pl.DeviceIdType.MESH
F32 = jnp.float32
BF16 = jnp.bfloat16

HEAD = 128
REACH = 64
NT = (((1,), (1,)), ((), ()))
TN = (((0,), (0,)), ((), ()))
ORDER = (10, 2, 8, 6, 14, 9, 11, 5, 15, 7, 13, 1, 3, 4, 12)


def kernel(
    clips, aq, ak, av, ao, fq, fo, fk, wg, wu, wd, gf,
    o_q, o_k, o_v, o_f, o_r,
    q_b, o_b, k_b, w_b, wd_b, f_b, aq_b, ao_b, kx, vx,
    gu, g_t, gtot, rx, cout, cin, ip, prx, psum, rsx,
    dq, dk_f, dv_f, dkv_s, dkv_r, f_t, bias, rate_s, rate_r, rate_o, fast_o, dk_o, dv_o,
    ld, halo_s, halo_r, a1_s, a1_r, a2_s, a2_r, pr_s, pr_r, rs_s, rs_r, dk_s, dk_r, rt_s, rt_r, st,
):
    tm, sp = lax.axis_index("tm"), lax.axis_index("space")
    mz, my = tm // 4, tm % 4
    mx, mk = sp // 2, sp % 2
    rows, hid = gf.shape
    feat = fq.shape[1]
    half = feat // 2
    tile = aq.shape[0]
    blk = hid // 8
    rt = 256

    barrier = pltpu.get_barrier_semaphore()
    for j in range(1, 16):
        pl.semaphore_signal(barrier, inc=1, device_id={"tm": lax.rem(tm + j, 16)}, device_id_type=MESH)
    for j in range(1, 8):
        pl.semaphore_signal(barrier, inc=1, device_id={"space": lax.rem(sp + j, 8)}, device_id_type=MESH)

    def load(i, src, dst):
        return pltpu.make_async_copy(src, dst, ld.at[i])

    first = [
        load(0, wg.at[0], w_b.at[:, pl.ds(0, hid)]),
        load(1, wu.at[0], w_b.at[:, pl.ds(hid, hid)]),
        load(2, fq, q_b),
        load(3, wd.at[0], wd_b),
        load(4, fo, o_b),
    ]
    later = [
        load(5, aq, aq_b),
        load(6, ao, ao_b),
        load(7, ak, kx.at[pl.ds(REACH, tile)]),
        load(8, av, vx.at[pl.ds(REACH, tile)]),
        load(9, fk, k_b),
        load(10, gf, f_b),
    ]
    for c in first:
        c.start()
    for c in later:
        c.start()

    left, right = lax.rem(sp + 7, 8), lax.rem(sp + 1, 8)

    def halo(i, src, dst, to):
        return pltpu.make_async_remote_copy(
            src_ref=src, dst_ref=dst, send_sem=halo_s.at[i], recv_sem=halo_r.at[i],
            device_id={"space": to}, device_id_type=MESH,
        )

    halos = [
        halo(0, ak.at[pl.ds(0, REACH)], kx.at[pl.ds(REACH + tile, REACH)], left),
        halo(1, av.at[pl.ds(0, REACH)], vx.at[pl.ds(REACH + tile, REACH)], left),
        halo(2, ak.at[pl.ds(tile - REACH, REACH)], kx.at[pl.ds(0, REACH)], right),
        halo(3, av.at[pl.ds(tile - REACH, REACH)], vx.at[pl.ds(0, REACH)], right),
    ]
    pl.semaphore_wait(barrier, 22)
    for c in halos:
        c.start()

    for c in first:
        c.wait()

    def rows_step(r, _):
        at = pl.ds(pl.multiple_of(r * rt, rt), rt)
        pre = jnp.dot(q_b[at, :], w_b[...], preferred_element_type=F32)
        hg = lax.dot_general(o_b[at, :], wd_b[...], NT, preferred_element_type=F32)
        gate, up = pre[:, :hid], pre[:, hid:]
        sig = 1.0 / (1.0 + jnp.exp(-gate))
        g = (hg * up * sig * (1.0 + gate * (1.0 - sig))).astype(BF16)
        gu[at, pl.ds(0, hid)] = g
        gu[at, pl.ds(hid, hid)] = (hg * (gate * sig)).astype(BF16)
        g_t[:, at] = g.T
        return 0

    lax.fori_loop(0, rows // rt, rows_step, 0)

    for h in range(2):
        def total_step(n, _):
            at = pl.ds(pl.multiple_of(n * 256, 256), 256)
            src = pl.ds(pl.multiple_of(h * half + n * 256, 256), 256)
            gtot[h, :, at] = jnp.dot(g_t[...], q_b[:, src], preferred_element_type=F32).astype(BF16)
            return 0

        lax.fori_loop(0, half // 256, total_step, 0)

    def peer(kk):
        dz, dy = kk // 4, kk % 4
        return lax.rem(mz + dz, 4) * 4 + lax.rem(my + dy, 4)

    def slice_of(ref, d):
        return ref.at[lax.rem(d, 2), pl.ds(pl.multiple_of((d // 2) * blk, 16), blk)]

    def out_copy(kk):
        d = peer(kk)
        return pltpu.make_async_remote_copy(
            src_ref=slice_of(gtot, d), dst_ref=rx.at[tm], send_sem=a1_s.at[kk], recv_sem=a1_r.at[kk],
            device_id={"tm": d}, device_id_type=MESH,
        )

    for kk in ORDER:
        out_copy(kk).start()
    rx[tm] = gtot[lax.rem(tm, 2), pl.ds(pl.multiple_of((tm // 2) * blk, 16), blk), :]

    def partner_copy(x):
        return pltpu.make_async_remote_copy(
            src_ref=ip.at[pl.ds(pl.multiple_of(x * 2 * tile + (1 - mk) * tile, tile), tile)], dst_ref=prx.at[x],
            send_sem=pr_s.at[x], recv_sem=pr_r.at[x],
            device_id={"space": mx * 2 + 1 - mk}, device_id_type=MESH,
        )

    def input_step(i, _):
        x = lax.rem(mx + 2 + i, 4)
        at = pl.ds(pl.multiple_of(x * rt, rt), rt)
        part = lax.dot_general(gu[at, :], w_b[...], NT, preferred_element_type=F32)
        ip[at, :] = part.astype(BF16)
        partner_copy(x).start()
        return 0

    lax.fori_loop(0, 4, input_step, 0)

    def rs_copy(dd):
        x = lax.rem(mx + dd, 4)
        return pltpu.make_async_remote_copy(
            src_ref=psum.at[x], dst_ref=rsx.at[dd], send_sem=rs_s.at[dd], recv_sem=rs_r.at[dd],
            device_id={"space": x * 2 + mk}, device_id_type=MESH,
        )

    def own_part(x):
        return ip[pl.ds(pl.multiple_of(x * 2 * tile + mk * tile, tile), tile), :].astype(F32)

    for dd in (2, 1, 3):
        x = lax.rem(mx + dd, 4)
        partner_copy(x).wait_recv()
        psum[x] = (own_part(x) + prx[x].astype(F32)).astype(BF16)
        rs_copy(dd).start()

    for c in later[:4]:
        c.wait()
    for c in halos:
        c.wait()
    key = lax.broadcasted_iota(jnp.int32, (2 * tile, tile), 0)
    query = lax.broadcasted_iota(jnp.int32, (2 * tile, tile), 1)
    apart = key - query
    place = key + (sp * tile - REACH)
    allowed = (apart >= 0) & (apart <= 2 * REACH) & (place >= 0) & (place < rows)
    bias[...] = jnp.where(allowed, 0.0, -1e30)
    scaling = 1.0 / math.sqrt(HEAD)

    def head_step(hh, _):
        at = pl.ds(pl.multiple_of(hh * HEAD, HEAD), HEAD)
        q, g, k, v = aq_b[:, at], ao_b[:, at], kx[:, at], vx[:, at]
        s = lax.dot_general(k, q, NT, preferred_element_type=F32) * scaling + bias[...]
        e = jnp.exp(s - jnp.max(s, axis=0, keepdims=True))
        p = e * (1.0 / jnp.sum(e, axis=0, keepdims=True))
        pb = p.astype(BF16)
        dp = lax.dot_general(v, g, NT, preferred_element_type=F32)
        delta = jnp.sum(pb.astype(F32) * dp, axis=0, keepdims=True)
        ds = (p * (dp - delta)).astype(BF16)
        dv = jnp.dot(pb, g, preferred_element_type=F32)
        dk = jnp.dot(ds, q, preferred_element_type=F32) * scaling
        dq[:, at] = (lax.dot_general(ds, k, TN, preferred_element_type=F32) * scaling).astype(BF16)
        dk_f[:, at] = dk[REACH : REACH + tile]
        dv_f[:, at] = dv[REACH : REACH + tile]
        dkv_s[0, 0, :, at] = dk[:REACH].astype(BF16)
        dkv_s[0, 1, :, at] = dv[:REACH].astype(BF16)
        dkv_s[1, 0, :, at] = dk[REACH + tile :].astype(BF16)
        dkv_s[1, 1, :, at] = dv[REACH + tile :].astype(BF16)
        return 0

    lax.fori_loop(0, aq.shape[1] // HEAD, head_step, 0)

    def back(i, to):
        return pltpu.make_async_remote_copy(
            src_ref=dkv_s.at[i], dst_ref=dkv_r.at[i], send_sem=dk_s.at[i], recv_sem=dk_r.at[i],
            device_id={"space": to}, device_id_type=MESH,
        )

    backs = [back(0, left), back(1, right)]
    for c in backs:
        c.start()
    store_q = pltpu.make_async_copy(dq, o_q, st.at[0])
    store_q.start()

    for c in later[4:]:
        c.wait()

    def turn_step(r, _):
        at = pl.ds(pl.multiple_of(r * rt, rt), rt)
        f_t[:, at] = f_b[at, :].T
        return 0

    lax.fori_loop(0, rows // rt, turn_step, 0)

    for kk in ORDER:
        out_copy(kk).wait_recv()
    s1 = clips[0]
    s2 = s1 + clips[1]
    s3 = s2 + clips[2]

    def scan_step(i, carry):
        c = 15 - i
        cout[c] = carry.astype(BF16)
        starts = (c == 0) | (c == s1) | (c == s2) | (c == s3)
        keep = jnp.where(starts, 0.0, 1.0).astype(F32)
        return keep * (carry + rx[c].astype(F32))

    lax.fori_loop(0, 16, scan_step, jnp.zeros((blk, half), F32))

    def carry_copy(kk):
        d = peer(kk)
        return pltpu.make_async_remote_copy(
            src_ref=cout.at[d], dst_ref=slice_of(cin, tm), send_sem=a2_s.at[kk], recv_sem=a2_r.at[kk],
            device_id={"tm": d}, device_id_type=MESH,
        )

    for kk in ORDER:
        carry_copy(kk).start()
    cin[lax.rem(tm, 2), pl.ds(pl.multiple_of((tm // 2) * blk, 16), blk), :] = cout[tm]

    partner_copy(mx).wait_recv()
    total = own_part(mx) + prx[mx].astype(F32)
    for dd in (1, 3, 2):
        rs_copy(dd).wait_recv()
        total = total + rsx[dd].astype(F32)
    fast_o[...] = total.astype(BF16)
    store_f = pltpu.make_async_copy(fast_o, o_f, st.at[1])
    store_f.start()

    for c in backs:
        c.wait_recv()
    dk_o[pl.ds(0, REACH), :] = (dk_f[pl.ds(0, REACH), :] + dkv_r[1, 0].astype(F32)).astype(BF16)
    dk_o[pl.ds(tile - REACH, REACH), :] = (dk_f[pl.ds(tile - REACH, REACH), :] + dkv_r[0, 0].astype(F32)).astype(BF16)
    dv_o[pl.ds(0, REACH), :] = (dv_f[pl.ds(0, REACH), :] + dkv_r[1, 1].astype(F32)).astype(BF16)
    dv_o[pl.ds(tile - REACH, REACH), :] = (dv_f[pl.ds(tile - REACH, REACH), :] + dkv_r[0, 1].astype(F32)).astype(BF16)
    store_k = pltpu.make_async_copy(dk_o, o_k, st.at[2])
    store_v = pltpu.make_async_copy(dv_o, o_v, st.at[3])
    store_k.start()
    store_v.start()

    for kk in ORDER:
        carry_copy(kk).wait_recv()

    def rate_step(r, _):
        at = pl.ds(pl.multiple_of(r * rt, rt), rt)
        kc = lax.dot_general(cin[0], k_b[at, pl.ds(0, half)], NT, preferred_element_type=F32)
        kc += lax.dot_general(cin[1], k_b[at, pl.ds(half, half)], NT, preferred_element_type=F32)
        line = jnp.sum(kc * f_t[:, at].astype(F32), axis=0, keepdims=True) * (1.0 / rows)
        rate_s[2 * r] = jnp.broadcast_to(line[:, :tile], (8, tile))
        rate_s[2 * r + 1] = jnp.broadcast_to(line[:, tile:], (8, tile))
        return 0

    lax.fori_loop(0, rows // rt, rate_step, 0)

    def rate_copy(j):
        d = lax.rem(sp + j, 8)
        return pltpu.make_async_remote_copy(
            src_ref=rate_s.at[d], dst_ref=rate_r.at[j], send_sem=rt_s.at[j], recv_sem=rt_r.at[j],
            device_id={"space": d}, device_id_type=MESH,
        )

    for j in range(1, 8):
        rate_copy(j).start()
    rate = rate_s[sp]
    for j in range(1, 8):
        rate_copy(j).wait_recv()
        rate = rate + rate_r[j]
    rate_o[...] = rate[0:1, :]
    store_r = pltpu.make_async_copy(rate_o, o_r, st.at[4])
    store_r.start()

    for kk in ORDER:
        out_copy(kk).wait_send()
        carry_copy(kk).wait_send()
    for x in range(4):
        partner_copy(x).wait_send()
    for dd in (1, 2, 3):
        rs_copy(dd).wait_send()
    for c in backs:
        c.wait_send()
    for j in range(1, 8):
        rate_copy(j).wait_send()
    for c in (store_q, store_f, store_k, store_v, store_r):
        c.wait()


def per_device(attn_query, attn_key, attn_value, attn_outgrad, fast_query, fast_outgrad, fast_key,
               gate_weights, up_weights, down_weights, gate_factor, clip_groups):
    tile, width = attn_query.shape
    rows, hid = gate_factor.shape
    feat = fast_query.shape[1]
    half, blk = feat // 2, hid // 8
    any_spec = pl.BlockSpec(memory_space=pl.ANY)
    dma = pltpu.SemaphoreType.DMA
    V = pltpu.VMEM
    outs = pl.pallas_call(
        kernel,
        out_shape=(
            jax.ShapeDtypeStruct((tile, width), BF16),
            jax.ShapeDtypeStruct((tile, width), BF16),
            jax.ShapeDtypeStruct((tile, width), BF16),
            jax.ShapeDtypeStruct((tile, feat), BF16),
            jax.ShapeDtypeStruct((1, tile), F32),
        ),
        in_specs=[pl.BlockSpec(memory_space=pltpu.SMEM)] + [any_spec] * 11,
        out_specs=(any_spec,) * 5,
        scratch_shapes=[
            V((rows, feat), BF16), V((rows, feat), BF16), V((rows, feat), BF16),
            V((feat, 2 * hid), BF16), V((hid, feat), BF16), V((rows, hid), BF16),
            V((tile, width), BF16), V((tile, width), BF16), V((2 * tile, width), BF16), V((2 * tile, width), BF16),
            V((rows, 2 * hid), BF16), V((hid, rows), BF16), V((2, hid, half), BF16),
            V((16, blk, half), BF16), V((16, blk, half), BF16), V((2, hid, half), BF16),
            V((rows, feat), BF16), V((4, tile, feat), BF16), V((4, tile, feat), BF16), V((4, tile, feat), BF16),
            V((tile, width), BF16), V((tile, width), F32), V((tile, width), F32),
            V((2, 2, REACH, width), BF16), V((2, 2, REACH, width), BF16),
            V((hid, rows), BF16), V((2 * tile, tile), F32),
            V((8, 8, tile), F32), V((8, 8, tile), F32), V((1, tile), F32),
            V((tile, feat), BF16), V((tile, width), BF16), V((tile, width), BF16),
            dma((11,)), dma((4,)), dma((4,)), dma((16,)), dma((16,)), dma((16,)), dma((16,)),
            dma((4,)), dma((4,)), dma((4,)), dma((4,)), dma((2,)), dma((2,)), dma((8,)), dma((8,)), dma((5,)),
        ],
        compiler_params=pltpu.CompilerParams(
            collective_id=0, has_side_effects=True, vmem_limit_bytes=60 * 1024 * 1024
        ),
    )(clip_groups, attn_query, attn_key, attn_value, attn_outgrad, fast_query, fast_outgrad, fast_key,
      gate_weights, up_weights, down_weights, gate_factor)
    return outs[0], outs[1], outs[2], outs[3], outs[4].reshape(tile)


def solution(mesh):
    both = ("tm", "space")
    return jax.shard_map(
        per_device,
        mesh=mesh,
        in_specs=(
            P(both, None), P(both, None), P(both, None), P(both, None),
            P("tm", None), P("tm", None), P("tm", None),
            P("tm", None, "space"), P("tm", None, "space"), P("tm", "space", None),
            P("tm", "space"), P(),
        ),
        out_specs=(P(both, None), P(both, None), P(both, None), P(both, None), P(both)),
        check_vma=False,
    )
```

```python
import functools
import math

import jax
import jax.numpy as jnp
from jax import lax
from jax.experimental import pallas as pl
from jax.experimental.pallas import tpu as pltpu
from jax.sharding import PartitionSpec as P

MESH = pl.DeviceIdType.MESH
F32 = jnp.float32
UNROLL = 2
BF16 = jnp.bfloat16

HEAD = 128
REACH = 64
NT = (((1,), (1,)), ((), ()))
TN = (((0,), (0,)), ((), ()))
ORDER = (10, 2, 8, 6, 14, 9, 11, 5, 15, 7, 13, 1, 3, 4, 12)


def kernel(
    clips, aq, ak, av, ao, fq, fo, fk, wg, wu, wd, gf,
    o_q, o_k, o_v, o_f, o_r,
    q_b, o_b, k_b, w_b, wd_b, f_b, aq_b, ao_b, kx, vx,
    gu, g_t, gtot, rx, cout, cin, ip, prx, psum, rsx,
    dk_f, dv_f, dkv_s, dkv_r, f_t, bias, rate_s, rate_r, line,
    ld, halo_s, halo_r, a1_s, a1_r, a2_s, a2_r, pr_s, pr_r, rs_s, rs_r, dk_s, dk_r, rt_s, rt_r,
):
    tm, sp = lax.axis_index("tm"), lax.axis_index("space")
    mz, my = tm // 4, tm % 4
    mx, mk = sp // 2, sp % 2
    rows, hid = gf.shape
    feat = fq.shape[1]
    half = feat // 2
    tile = aq.shape[0]
    blk = hid // 8
    quarter = half // 2
    rt = 256

    barrier = pltpu.get_barrier_semaphore()
    for j in range(1, 16):
        pl.semaphore_signal(barrier, inc=1, device_id={"tm": lax.rem(tm + j, 16)}, device_id_type=MESH)
    for j in range(1, 8):
        pl.semaphore_signal(barrier, inc=1, device_id={"space": lax.rem(sp + j, 8)}, device_id_type=MESH)

    def load(i, src, dst):
        return pltpu.make_async_copy(src, dst, ld.at[i])

    weights = [
        load(0, wg.at[0], w_b.at[:, pl.ds(0, hid)]),
        load(1, wu.at[0], w_b.at[:, pl.ds(hid, hid)]),
        load(2, wd.at[0], wd_b),
    ]

    def block(r):
        return pl.ds(pl.multiple_of(r * rt, rt), rt)

    def inputs(r):
        return [
            load(3 + r, fq.at[block(r)], q_b.at[block(r)]),
            load(7 + r, fo.at[block(r)], o_b.at[block(r)]),
        ]

    later = [
        load(11, aq, aq_b),
        load(12, ao, ao_b),
        load(13, ak, kx.at[pl.ds(REACH, tile)]),
        load(14, av, vx.at[pl.ds(REACH, tile)]),
        load(15, fk, k_b),
        load(16, gf, f_b),
    ]
    for c in weights:
        c.start()
    for r in range(4):
        for c in inputs(r):
            c.start()

    left, right = lax.rem(sp + 7, 8), lax.rem(sp + 1, 8)

    def halo(i, src, dst, to):
        return pltpu.make_async_remote_copy(
            src_ref=src, dst_ref=dst, send_sem=halo_s.at[i], recv_sem=halo_r.at[i],
            device_id={"space": to}, device_id_type=MESH,
        )

    halos = [
        halo(0, ak.at[pl.ds(0, REACH)], kx.at[pl.ds(REACH + tile, REACH)], left),
        halo(1, av.at[pl.ds(0, REACH)], vx.at[pl.ds(REACH + tile, REACH)], left),
        halo(2, ak.at[pl.ds(tile - REACH, REACH)], kx.at[pl.ds(0, REACH)], right),
        halo(3, av.at[pl.ds(tile - REACH, REACH)], vx.at[pl.ds(0, REACH)], right),
    ]
    pl.semaphore_wait(barrier, 22)
    for c in halos:
        c.start()

    def peer(kk):
        dz, dy = kk // 4, kk % 4
        return lax.rem(mz + dz, 4) * 4 + lax.rem(my + dy, 4)

    def slice_of(ref, n, d):
        down, over = pl.multiple_of((d // 2) * blk, 16), pl.multiple_of(lax.rem(d, 2) * quarter, 128)
        return ref.at[n, pl.ds(down, blk), pl.ds(over, quarter)]

    def out_copy(n, kk):
        d = peer(kk)
        return pltpu.make_async_remote_copy(
            src_ref=slice_of(gtot, n, d), dst_ref=rx.at[n, tm],
            send_sem=a1_s.at[n * 16 + kk], recv_sem=a1_r.at[n * 16 + kk],
            device_id={"tm": d}, device_id_type=MESH,
        )

    def carry_copy(n, kk):
        d = peer(kk)
        return pltpu.make_async_remote_copy(
            src_ref=cout.at[n, d], dst_ref=slice_of(cin, n, tm),
            send_sem=a2_s.at[n * 16 + kk], recv_sem=a2_r.at[n * 16 + kk],
            device_id={"tm": d}, device_id_type=MESH,
        )

    for c in weights:
        c.wait()

    def rows_step(r, _):
        at = block(r)
        for c in inputs(r):
            c.wait()
        pre = jnp.dot(q_b[at, :], w_b[...], preferred_element_type=F32)
        hg = lax.dot_general(o_b[at, :], wd_b[...], NT, preferred_element_type=F32)
        gate, up = pre[:, :hid], pre[:, hid:]
        sig = 1.0 / (1.0 + jnp.exp(-gate))
        g = (hg * up * sig * (1.0 + gate * (1.0 - sig))).astype(BF16)
        gu[at, pl.ds(0, hid)] = g
        gu[at, pl.ds(hid, hid)] = (hg * (gate * sig)).astype(BF16)
        g_t[:, at] = g.T
        return 0

    lax.fori_loop(0, rows // rt, rows_step, 0)
    for c in later:
        c.start()

    for n in range(2):
        def total_step(i, _, n=n):
            at = pl.ds(pl.multiple_of(i * 256, 256), 256)
            src = pl.ds(pl.multiple_of(n * half + i * 256, 256), 256)
            gtot[n, :, at] = jnp.dot(g_t[...], q_b[:, src], preferred_element_type=F32).astype(BF16)
            return 0

        lax.fori_loop(0, half // 256, total_step, 0)
        for kk in ORDER:
            out_copy(n, kk).start()
        rx[n, tm] = slice_of(gtot, n, tm)[...]

    s1 = clips[0]
    s2 = s1 + clips[1]
    s3 = s2 + clips[2]

    def carries(n):
        for kk in ORDER:
            out_copy(n, kk).wait_recv()

        def scan_step(i, carry):
            c = 15 - i
            cout[n, c] = carry.astype(BF16)
            starts = (c == 0) | (c == s1) | (c == s2) | (c == s3)
            keep = jnp.where(starts, 0.0, 1.0).astype(F32)
            return keep * (carry + rx[n, c].astype(F32))

        lax.fori_loop(0, 16, scan_step, jnp.zeros((blk, quarter), F32))
        for kk in ORDER:
            carry_copy(n, kk).start()
        slice_of(cin, n, tm)[...] = cout[n, tm]

    def partner_copy(x):
        return pltpu.make_async_remote_copy(
            src_ref=ip.at[pl.ds(pl.multiple_of(x * 2 * tile + (1 - mk) * tile, tile), tile)], dst_ref=prx.at[x],
            send_sem=pr_s.at[x], recv_sem=pr_r.at[x],
            device_id={"space": mx * 2 + 1 - mk}, device_id_type=MESH,
        )

    def input_step(i, _):
        x = lax.rem(mx + 2 + i, 4)
        at = pl.ds(pl.multiple_of(x * rt, rt), rt)
        terms = lax.dot_general(gu[at, :], w_b[...], NT, preferred_element_type=F32)
        ip[at, :] = terms.astype(BF16)
        partner_copy(x).start()
        return 0

    lax.fori_loop(0, 4, input_step, 0)

    ahead, behind = 1 + 2 * mk, 3 - 2 * mk

    def rs_copy(i, to):
        return pltpu.make_async_remote_copy(
            src_ref=psum.at[i], dst_ref=rsx.at[i], send_sem=rs_s.at[i], recv_sem=rs_r.at[i],
            device_id={"space": lax.rem(mx + to, 4) * 2 + mk}, device_id_type=MESH,
        )

    relay = [rs_copy(0, ahead), rs_copy(1, ahead), rs_copy(2, behind)]

    def pair_sum(to):
        x = lax.rem(mx + to, 4)
        partner_copy(x).wait_recv()
        mine = ip[pl.ds(pl.multiple_of(x * 2 * tile + mk * tile, tile), tile), :]
        return mine.astype(F32) + prx[x].astype(F32)

    psum[0] = pair_sum(2).astype(BF16)
    relay[0].start()
    psum[2] = pair_sum(behind).astype(BF16)
    relay[2].start()

    for c in later[:4]:
        c.wait()
    for c in halos:
        c.wait()
    key = lax.broadcasted_iota(jnp.int32, (2 * tile, tile), 0)
    query = lax.broadcasted_iota(jnp.int32, (2 * tile, tile), 1)
    apart = key - query
    place = key + (sp * tile - REACH)
    allowed = (apart >= 0) & (apart <= 2 * REACH) & (place >= 0) & (place < rows)
    bias[...] = jnp.where(allowed, 0.0, -1e30)
    scaling = 1.0 / math.sqrt(HEAD)

    def one_head(hh):
        at = pl.ds(pl.multiple_of(hh * HEAD, HEAD), HEAD)
        q, g, k, v = aq_b[:, at], ao_b[:, at], kx[:, at], vx[:, at]
        s = lax.dot_general(k, q, NT, preferred_element_type=F32) * (scaling * math.log2(math.e)) + bias[...]
        e = jnp.exp2(s - jnp.max(s, axis=0, keepdims=True))
        p = e * (1.0 / jnp.sum(e, axis=0, keepdims=True))
        pb = p.astype(BF16)
        dp = lax.dot_general(v, g, NT, preferred_element_type=F32)
        delta = jnp.sum(pb.astype(F32) * dp, axis=0, keepdims=True)
        ds = (p * (dp - delta)).astype(BF16)
        dv = jnp.dot(pb, g, preferred_element_type=F32)
        dk = jnp.dot(ds, q, preferred_element_type=F32) * scaling
        o_q[:, at] = (lax.dot_general(ds, k, TN, preferred_element_type=F32) * scaling).astype(BF16)
        dk_f[:, at] = dk[REACH : REACH + tile]
        dv_f[:, at] = dv[REACH : REACH + tile]
        dkv_s[0, 0, :, at] = dk[:REACH].astype(BF16)
        dkv_s[0, 1, :, at] = dv[:REACH].astype(BF16)
        dkv_s[1, 0, :, at] = dk[REACH + tile :].astype(BF16)
        dkv_s[1, 1, :, at] = dv[REACH + tile :].astype(BF16)

    def head_step(i, _):
        for j in range(UNROLL):
            one_head(i * UNROLL + j)
        return 0

    steps = aq.shape[1] // HEAD // UNROLL
    lax.fori_loop(0, steps // 2, head_step, 0)
    relay[0].wait_recv()
    psum[1] = (pair_sum(ahead) + rsx[0].astype(F32)).astype(BF16)
    relay[1].start()
    carries(0)
    lax.fori_loop(steps // 2, steps, head_step, 0)

    def back(i, to):
        return pltpu.make_async_remote_copy(
            src_ref=dkv_s.at[i], dst_ref=dkv_r.at[i], send_sem=dk_s.at[i], recv_sem=dk_r.at[i],
            device_id={"space": to}, device_id_type=MESH,
        )

    backs = [back(0, left), back(1, right)]
    for c in backs:
        c.start()

    for c in later[4:]:
        c.wait()

    def turn_step(r, _):
        at = pl.ds(pl.multiple_of(r * rt, rt), rt)
        f_t[:, at] = f_b[at, :].T
        return 0

    lax.fori_loop(0, rows // rt, turn_step, 0)

    carries(1)

    total = pair_sum(0)
    for i in (2, 1):
        relay[i].wait_recv()
        total = total + rsx[i].astype(F32)
    o_f[...] = total.astype(BF16)

    for c in backs:
        c.wait_recv()
    o_k[pl.ds(0, REACH), :] = (dk_f[pl.ds(0, REACH), :] + dkv_r[1, 0].astype(F32)).astype(BF16)
    o_k[pl.ds(tile - REACH, REACH), :] = (dk_f[pl.ds(tile - REACH, REACH), :] + dkv_r[0, 0].astype(F32)).astype(BF16)
    o_v[pl.ds(0, REACH), :] = (dv_f[pl.ds(0, REACH), :] + dkv_r[1, 1].astype(F32)).astype(BF16)
    o_v[pl.ds(tile - REACH, REACH), :] = (dv_f[pl.ds(tile - REACH, REACH), :] + dkv_r[0, 1].astype(F32)).astype(BF16)

    for n in range(2):
        for kk in ORDER:
            carry_copy(n, kk).wait_recv()

        def rate_step(r, _, n=n):
            at = block(r)
            kc = lax.dot_general(cin[n], k_b[at, pl.ds(n * half, half)], NT, preferred_element_type=F32)
            more = jnp.sum(kc * f_t[:, at].astype(F32), axis=0, keepdims=True)
            if n == 0:
                line[r] = more
            else:
                more = (line[r] + more) * (1.0 / rows)
                rate_s[2 * r] = jnp.broadcast_to(more[:, :tile], (8, tile))
                rate_s[2 * r + 1] = jnp.broadcast_to(more[:, tile:], (8, tile))
            return 0

        lax.fori_loop(0, rows // rt, rate_step, 0)

    def rate_copy(j):
        d = lax.rem(sp + j, 8)
        return pltpu.make_async_remote_copy(
            src_ref=rate_s.at[d], dst_ref=rate_r.at[j], send_sem=rt_s.at[j], recv_sem=rt_r.at[j],
            device_id={"space": d}, device_id_type=MESH,
        )

    for j in range(1, 8):
        rate_copy(j).start()
    rate = rate_s[sp]
    for j in range(1, 8):
        rate_copy(j).wait_recv()
        rate = rate + rate_r[j]
    o_r[...] = rate[0:1, :]

    for kk in ORDER:
        for n in range(2):
            out_copy(n, kk).wait_send()
            carry_copy(n, kk).wait_send()
    for x in range(4):
        partner_copy(x).wait_send()
    for c in relay:
        c.wait_send()
    for c in backs:
        c.wait_send()
    for j in range(1, 8):
        rate_copy(j).wait_send()


def put_out(a, b, c, d, e, oa, ob, oc, od, oe, sem):
    copies = [pltpu.make_async_copy(src, dst, sem.at[i])
              for i, (src, dst) in enumerate(((a, oa), (b, ob), (c, oc), (d, od), (e, oe)))]
    for c in copies:
        c.start()
    for c in copies:
        c.wait()


def per_device(attn_query, attn_key, attn_value, attn_outgrad, fast_query, fast_outgrad, fast_key,
               gate_weights, up_weights, down_weights, gate_factor, clip_groups):
    tile, width = attn_query.shape
    rows, hid = gate_factor.shape
    feat = fast_query.shape[1]
    half, blk = feat // 2, hid // 8
    any_spec = pl.BlockSpec(memory_space=pl.ANY)
    dma = pltpu.SemaphoreType.DMA
    V = pltpu.VMEM
    outs = pl.pallas_call(
        kernel,
        out_shape=(
            V((tile, width), BF16), V((tile, width), BF16), V((tile, width), BF16),
            V((tile, feat), BF16), V((1, tile), F32),
        ),
        in_specs=[pl.BlockSpec(memory_space=pltpu.SMEM)] + [any_spec] * 11,
        out_specs=(pl.BlockSpec(memory_space=V),) * 5,
        scratch_shapes=[
            V((rows, feat), BF16), V((rows, feat), BF16), V((rows, feat), BF16),
            V((feat, 2 * hid), BF16), V((hid, feat), BF16), V((rows, hid), BF16),
            V((tile, width), BF16), V((tile, width), BF16), V((2 * tile, width), BF16), V((2 * tile, width), BF16),
            V((rows, 2 * hid), BF16), V((hid, rows), BF16), V((2, hid, half), BF16),
            V((2, 16, blk, half // 2), BF16), V((2, 16, blk, half // 2), BF16), V((2, hid, half), BF16),
            V((rows, feat), BF16), V((4, tile, feat), BF16), V((3, tile, feat), BF16), V((3, tile, feat), BF16),
            V((tile, width), F32), V((tile, width), F32),
            V((2, 2, REACH, width), BF16), V((2, 2, REACH, width), BF16),
            V((hid, rows), BF16), V((2 * tile, tile), F32),
            V((8, 8, tile), F32), V((8, 8, tile), F32), V((4, 1, 256), F32),
            dma((17,)), dma((4,)), dma((4,)), dma((32,)), dma((32,)), dma((32,)), dma((32,)),
            dma((4,)), dma((4,)), dma((3,)), dma((3,)), dma((2,)), dma((2,)), dma((8,)), dma((8,)),
        ],
        compiler_params=pltpu.CompilerParams(
            collective_id=0, has_side_effects=True, vmem_limit_bytes=64_500_000
        ),
    )(clip_groups, attn_query, attn_key, attn_value, attn_outgrad, fast_query, fast_outgrad, fast_key,
      gate_weights, up_weights, down_weights, gate_factor)
    outs = pl.pallas_call(
        put_out,
        out_shape=tuple(jax.ShapeDtypeStruct(o.shape, o.dtype) for o in outs),
        in_specs=[pl.BlockSpec(memory_space=V)] * 5,
        out_specs=(any_spec,) * 5,
        scratch_shapes=[dma((5,))],
        compiler_params=pltpu.CompilerParams(vmem_limit_bytes=1024 * 1024),
    )(*outs)
    return outs[0], outs[1], outs[2], outs[3], outs[4].reshape(tile)


def solution(mesh):
    both = ("tm", "space")
    return jax.shard_map(
        per_device,
        mesh=mesh,
        in_specs=(
            P(both, None), P(both, None), P(both, None), P(both, None),
            P("tm", None), P("tm", None), P("tm", None),
            P("tm", None, "space"), P("tm", None, "space"), P("tm", "space", None),
            P("tm", "space"), P(),
        ),
        out_specs=(P(both, None), P(both, None), P(both, None), P(both, None), P(both)),
        check_vma=False,
    )
```

```python
import functools
import math

import jax
import jax.numpy as jnp
from jax import lax
from jax.experimental import pallas as pl
from jax.experimental.pallas import tpu as pltpu
from jax.sharding import PartitionSpec as P

MESH = pl.DeviceIdType.MESH
F32 = jnp.float32
UNROLL = 5
BF16 = jnp.bfloat16

HEAD = 128
REACH = 64
NT = (((1,), (1,)), ((), ()))
TN = (((0,), (0,)), ((), ()))
ORDER = (10, 2, 8, 6, 14, 9, 11, 5, 15, 7, 13, 1, 3, 4, 12)


def kernel(
    clips, aq, ak, av, ao, fq, fo, fk, wg, wu, wd, gf,
    o_q, o_k, o_v, o_f, o_r,
    q_b, o_b, k_b, w_b, wd_b, f_b, aq_b, ao_b, kx, vx,
    gu, g_t, gtot, rx, cout, cin, ip, prx, psum, rsx,
    dk_f, dv_f, dkv_s, dkv_r, f_t, bias, rate_s, rate_r, line,
    ld, halo_s, halo_r, a1_s, a1_r, a2_s, a2_r, pr_s, pr_r, rs_s, rs_r, dk_s, dk_r, rt_s, rt_r,
):
    tm, sp = lax.axis_index("tm"), lax.axis_index("space")
    mz, my = tm // 4, tm % 4
    mx, mk = sp // 2, sp % 2
    rows, hid = gf.shape
    feat = fq.shape[1]
    half = feat // 2
    tile = aq.shape[0]
    blk = hid // 8
    quarter = half // 2
    rt = 256

    barrier = pltpu.get_barrier_semaphore()
    for j in range(1, 16):
        pl.semaphore_signal(barrier, inc=1, device_id={"tm": lax.rem(tm + j, 16)}, device_id_type=MESH)
    for j in range(1, 8):
        pl.semaphore_signal(barrier, inc=1, device_id={"space": lax.rem(sp + j, 8)}, device_id_type=MESH)

    def load(i, src, dst):
        return pltpu.make_async_copy(src, dst, ld.at[i])

    weights = [
        load(0, wg.at[0], w_b.at[:, pl.ds(0, hid)]),
        load(1, wu.at[0], w_b.at[:, pl.ds(hid, hid)]),
        load(2, wd.at[0], wd_b),
    ]

    def block(r):
        return pl.ds(pl.multiple_of(r * rt, rt), rt)

    def inputs(r):
        return [
            load(3 + r, fq.at[block(r)], q_b.at[block(r)]),
            load(7 + r, fo.at[block(r)], o_b.at[block(r)]),
        ]

    later = [
        load(11, aq, aq_b),
        load(12, ao, ao_b),
        load(13, ak, kx.at[pl.ds(REACH, tile)]),
        load(14, av, vx.at[pl.ds(REACH, tile)]),
        load(15, fk, k_b),
        load(16, gf, f_b),
    ]
    for c in weights:
        c.start()
    for r in range(4):
        for c in inputs(r):
            c.start()

    left, right = lax.rem(sp + 7, 8), lax.rem(sp + 1, 8)

    def halo(i, src, dst, to):
        return pltpu.make_async_remote_copy(
            src_ref=src, dst_ref=dst, send_sem=halo_s.at[i], recv_sem=halo_r.at[i],
            device_id={"space": to}, device_id_type=MESH,
        )

    halos = [
        halo(0, ak.at[pl.ds(0, REACH)], kx.at[pl.ds(REACH + tile, REACH)], left),
        halo(1, av.at[pl.ds(0, REACH)], vx.at[pl.ds(REACH + tile, REACH)], left),
        halo(2, ak.at[pl.ds(tile - REACH, REACH)], kx.at[pl.ds(0, REACH)], right),
        halo(3, av.at[pl.ds(tile - REACH, REACH)], vx.at[pl.ds(0, REACH)], right),
    ]

    def peer(kk):
        dz, dy = kk // 4, kk % 4
        return lax.rem(mz + dz, 4) * 4 + lax.rem(my + dy, 4)

    def slice_of(ref, n, d):
        down, over = pl.multiple_of((d // 2) * blk, 16), pl.multiple_of(lax.rem(d, 2) * quarter, 128)
        return ref.at[n, pl.ds(down, blk), pl.ds(over, quarter)]

    def out_copy(n, kk):
        d = peer(kk)
        return pltpu.make_async_remote_copy(
            src_ref=slice_of(gtot, n, d), dst_ref=rx.at[n, tm],
            send_sem=a1_s.at[n * 16 + kk], recv_sem=a1_r.at[n * 16 + kk],
            device_id={"tm": d}, device_id_type=MESH,
        )

    def carry_copy(n, kk):
        d = peer(kk)
        return pltpu.make_async_remote_copy(
            src_ref=cout.at[n, d], dst_ref=slice_of(cin, n, tm),
            send_sem=a2_s.at[n * 16 + kk], recv_sem=a2_r.at[n * 16 + kk],
            device_id={"tm": d}, device_id_type=MESH,
        )

    for c in weights:
        c.wait()

    def rows_step(r, _):
        at = block(r)
        for c in inputs(r):
            c.wait()
        pre = jnp.dot(q_b[at, :], w_b[...], preferred_element_type=F32)
        hg = lax.dot_general(o_b[at, :], wd_b[...], NT, preferred_element_type=F32)
        gate, up = pre[:, :hid], pre[:, hid:]
        sig = 1.0 / (1.0 + jnp.exp(-gate))
        g = (hg * up * sig * (1.0 + gate * (1.0 - sig))).astype(BF16)
        gu[at, pl.ds(0, hid)] = g
        gu[at, pl.ds(hid, hid)] = (hg * (gate * sig)).astype(BF16)
        g_t[:, at] = g.T
        return 0

    lax.fori_loop(0, 2, rows_step, 0)
    pl.semaphore_wait(barrier, 22)
    for c in halos:
        c.start()
    lax.fori_loop(2, rows // rt, rows_step, 0)
    for c in later:
        c.start()

    for n in range(2):
        def total_step(i, _, n=n):
            at = pl.ds(pl.multiple_of(i * 256, 256), 256)
            src = pl.ds(pl.multiple_of(n * half + i * 256, 256), 256)
            gtot[n, :, at] = jnp.dot(g_t[...], q_b[:, src], preferred_element_type=F32).astype(BF16)
            return 0

        lax.fori_loop(0, half // 256, total_step, 0)
        for kk in ORDER:
            out_copy(n, kk).start()
        rx[n, tm] = slice_of(gtot, n, tm)[...]

    s1 = clips[0]
    s2 = s1 + clips[1]
    s3 = s2 + clips[2]

    def carries(n):
        for kk in ORDER:
            out_copy(n, kk).wait_recv()

        def scan_step(i, carry):
            c = 15 - i
            cout[n, c] = carry.astype(BF16)
            starts = (c == 0) | (c == s1) | (c == s2) | (c == s3)
            keep = jnp.where(starts, 0.0, 1.0).astype(F32)
            return keep * (carry + rx[n, c].astype(F32))

        lax.fori_loop(0, 16, scan_step, jnp.zeros((blk, quarter), F32))
        for kk in ORDER:
            carry_copy(n, kk).start()
        slice_of(cin, n, tm)[...] = cout[n, tm]

    def partner_copy(x):
        return pltpu.make_async_remote_copy(
            src_ref=ip.at[pl.ds(pl.multiple_of(x * 2 * tile + (1 - mk) * tile, tile), tile)], dst_ref=prx.at[x],
            send_sem=pr_s.at[x], recv_sem=pr_r.at[x],
            device_id={"space": mx * 2 + 1 - mk}, device_id_type=MESH,
        )

    def input_step(i, _):
        x = lax.rem(mx + 2 + i, 4)
        at = pl.ds(pl.multiple_of(x * rt, rt), rt)
        terms = lax.dot_general(gu[at, :], w_b[...], NT, preferred_element_type=F32)
        ip[at, :] = terms.astype(BF16)
        partner_copy(x).start()
        return 0

    lax.fori_loop(0, 4, input_step, 0)

    ahead, behind = 1 + 2 * mk, 3 - 2 * mk

    def rs_copy(i, to):
        return pltpu.make_async_remote_copy(
            src_ref=psum.at[i], dst_ref=rsx.at[i], send_sem=rs_s.at[i], recv_sem=rs_r.at[i],
            device_id={"space": lax.rem(mx + to, 4) * 2 + mk}, device_id_type=MESH,
        )

    relay = [rs_copy(0, ahead), rs_copy(1, ahead), rs_copy(2, behind)]

    def pair_sum(to):
        x = lax.rem(mx + to, 4)
        partner_copy(x).wait_recv()
        mine = ip[pl.ds(pl.multiple_of(x * 2 * tile + mk * tile, tile), tile), :]
        return mine.astype(F32) + prx[x].astype(F32)

    psum[0] = pair_sum(2).astype(BF16)
    relay[0].start()
    psum[2] = pair_sum(behind).astype(BF16)
    relay[2].start()

    for c in later[:4]:
        c.wait()
    for c in halos:
        c.wait()
    key = lax.broadcasted_iota(jnp.int32, (2 * tile, tile), 0)
    query = lax.broadcasted_iota(jnp.int32, (2 * tile, tile), 1)
    apart = key - query
    place = key + (sp * tile - REACH)
    allowed = (apart >= 0) & (apart <= 2 * REACH) & (place >= 0) & (place < rows)
    bias[...] = jnp.where(allowed, 0.0, -1e30)
    scaling = 1.0 / math.sqrt(HEAD)

    def one_head(hh):
        at = pl.ds(pl.multiple_of(hh * HEAD, HEAD), HEAD)
        q, g, k, v = aq_b[:, at], ao_b[:, at], kx[:, at], vx[:, at]
        s = lax.dot_general(k, q, NT, preferred_element_type=F32) * (scaling * math.log2(math.e)) + bias[...]
        e = jnp.exp2(s - jnp.max(s, axis=0, keepdims=True))
        p = e * (1.0 / jnp.sum(e, axis=0, keepdims=True))
        pb = p.astype(BF16)
        dp = lax.dot_general(v, g, NT, preferred_element_type=F32)
        delta = jnp.sum(pb.astype(F32) * dp, axis=0, keepdims=True)
        ds = (p * (dp - delta)).astype(BF16)
        dv = jnp.dot(pb, g, preferred_element_type=F32)
        dk = jnp.dot(ds, q, preferred_element_type=F32) * scaling
        o_q[:, at] = (lax.dot_general(ds, k, TN, preferred_element_type=F32) * scaling).astype(BF16)
        dk_f[:, at] = dk[REACH : REACH + tile]
        dv_f[:, at] = dv[REACH : REACH + tile]
        dkv_s[0, 0, :, at] = dk[:REACH].astype(BF16)
        dkv_s[0, 1, :, at] = dv[:REACH].astype(BF16)
        dkv_s[1, 0, :, at] = dk[REACH + tile :].astype(BF16)
        dkv_s[1, 1, :, at] = dv[REACH + tile :].astype(BF16)

    def head_step(i, _):
        for j in range(UNROLL):
            one_head(i * UNROLL + j)
        return 0

    steps = aq.shape[1] // HEAD // UNROLL
    lax.fori_loop(0, steps // 2, head_step, 0)
    carries(0)
    lax.fori_loop(steps // 2, steps, head_step, 0)

    def back(i, to):
        return pltpu.make_async_remote_copy(
            src_ref=dkv_s.at[i], dst_ref=dkv_r.at[i], send_sem=dk_s.at[i], recv_sem=dk_r.at[i],
            device_id={"space": to}, device_id_type=MESH,
        )

    backs = [back(0, left), back(1, right)]
    for c in backs:
        c.start()
    relay[0].wait_recv()
    psum[1] = (pair_sum(ahead) + rsx[0].astype(F32)).astype(BF16)
    relay[1].start()

    for c in later[4:]:
        c.wait()

    def turn_step(r, _):
        at = pl.ds(pl.multiple_of(r * rt, rt), rt)
        f_t[:, at] = f_b[at, :].T
        return 0

    lax.fori_loop(0, rows // rt, turn_step, 0)

    carries(1)

    def rate_copy(d):
        j = lax.rem(d - sp + 8, 8)
        return pltpu.make_async_remote_copy(
            src_ref=rate_s.at[d], dst_ref=rate_r.at[j], send_sem=rt_s.at[j], recv_sem=rt_r.at[j],
            device_id={"space": d}, device_id_type=MESH,
        )

    def rate_part(n, r):
        at = block(r)
        kc = lax.dot_general(cin[n], k_b[at, pl.ds(n * half, half)], NT, preferred_element_type=F32)
        return jnp.sum(kc * f_t[:, at].astype(F32), axis=0, keepdims=True)

    def rate_first(r, _):
        line[r] = rate_part(0, r)
        return 0

    def rate_second(r):
        whole = (line[r] + rate_part(1, r)) * (1.0 / rows)
        rate_s[2 * r] = jnp.broadcast_to(whole[:, :tile], (8, tile))
        rate_s[2 * r + 1] = jnp.broadcast_to(whole[:, tile:], (8, tile))

    for kk in ORDER:
        carry_copy(0, kk).wait_recv()
    lax.fori_loop(0, rows // rt, rate_first, 0)

    total = pair_sum(0)
    for i in (2, 1):
        relay[i].wait_recv()
        total = total + rsx[i].astype(F32)
    o_f[...] = total.astype(BF16)

    for c in backs:
        c.wait_recv()
    o_k[pl.ds(0, REACH), :] = (dk_f[pl.ds(0, REACH), :] + dkv_r[1, 0].astype(F32)).astype(BF16)
    o_k[pl.ds(tile - REACH, REACH), :] = (dk_f[pl.ds(tile - REACH, REACH), :] + dkv_r[0, 0].astype(F32)).astype(BF16)
    o_v[pl.ds(0, REACH), :] = (dv_f[pl.ds(0, REACH), :] + dkv_r[1, 1].astype(F32)).astype(BF16)
    o_v[pl.ds(tile - REACH, REACH), :] = (dv_f[pl.ds(tile - REACH, REACH), :] + dkv_r[0, 1].astype(F32)).astype(BF16)

    for kk in ORDER:
        carry_copy(1, kk).wait_recv()

    def rate_away(i):
        r = lax.rem(mx + 2 + i, 4)
        rate_second(r)
        rate_copy(2 * r).start()
        rate_copy(2 * r + 1).start()

    for i in (0, 1, 3):
        rate_away(i)
    rate_second(mx)
    rate_copy(2 * mx + 1 - mk).start()
    rate = rate_s[sp]
    for j in range(1, 8):
        rate_copy(lax.rem(sp + j, 8)).wait_recv()
        rate = rate + rate_r[j]
    o_r[...] = rate[0:1, :]

    for kk in ORDER:
        for n in range(2):
            out_copy(n, kk).wait_send()
            carry_copy(n, kk).wait_send()
    for x in range(4):
        partner_copy(x).wait_send()
    for c in relay:
        c.wait_send()
    for c in backs:
        c.wait_send()
    for j in range(1, 8):
        rate_copy(lax.rem(sp + j, 8)).wait_send()


def put_out(a, b, c, d, e, oa, ob, oc, od, oe, sem):
    copies = [pltpu.make_async_copy(src, dst, sem.at[i])
              for i, (src, dst) in enumerate(((a, oa), (b, ob), (c, oc), (d, od), (e, oe)))]
    for c in copies:
        c.start()
    for c in copies:
        c.wait()


def per_device(attn_query, attn_key, attn_value, attn_outgrad, fast_query, fast_outgrad, fast_key,
               gate_weights, up_weights, down_weights, gate_factor, clip_groups):
    tile, width = attn_query.shape
    rows, hid = gate_factor.shape
    feat = fast_query.shape[1]
    half, blk = feat // 2, hid // 8
    any_spec = pl.BlockSpec(memory_space=pl.ANY)
    dma = pltpu.SemaphoreType.DMA
    V = pltpu.VMEM
    outs = pl.pallas_call(
        kernel,
        out_shape=(
            V((tile, width), BF16), V((tile, width), BF16), V((tile, width), BF16),
            V((tile, feat), BF16), V((1, tile), F32),
        ),
        in_specs=[pl.BlockSpec(memory_space=pltpu.SMEM)] + [any_spec] * 11,
        out_specs=(pl.BlockSpec(memory_space=V),) * 5,
        scratch_shapes=[
            V((rows, feat), BF16), V((rows, feat), BF16), V((rows, feat), BF16),
            V((feat, 2 * hid), BF16), V((hid, feat), BF16), V((rows, hid), BF16),
            V((tile, width), BF16), V((tile, width), BF16), V((2 * tile, width), BF16), V((2 * tile, width), BF16),
            V((rows, 2 * hid), BF16), V((hid, rows), BF16), V((2, hid, half), BF16),
            V((2, 16, blk, half // 2), BF16), V((2, 16, blk, half // 2), BF16), V((2, hid, half), BF16),
            V((rows, feat), BF16), V((4, tile, feat), BF16), V((3, tile, feat), BF16), V((3, tile, feat), BF16),
            V((tile, width), F32), V((tile, width), F32),
            V((2, 2, REACH, width), BF16), V((2, 2, REACH, width), BF16),
            V((hid, rows), BF16), V((2 * tile, tile), F32),
            V((8, 8, tile), F32), V((8, 8, tile), F32), V((4, 1, 256), F32),
            dma((17,)), dma((4,)), dma((4,)), dma((32,)), dma((32,)), dma((32,)), dma((32,)),
            dma((4,)), dma((4,)), dma((3,)), dma((3,)), dma((2,)), dma((2,)), dma((8,)), dma((8,)),
        ],
        compiler_params=pltpu.CompilerParams(
            collective_id=0, has_side_effects=True, vmem_limit_bytes=64_500_000
        ),
    )(clip_groups, attn_query, attn_key, attn_value, attn_outgrad, fast_query, fast_outgrad, fast_key,
      gate_weights, up_weights, down_weights, gate_factor)
    outs = pl.pallas_call(
        put_out,
        out_shape=tuple(jax.ShapeDtypeStruct(o.shape, o.dtype) for o in outs),
        in_specs=[pl.BlockSpec(memory_space=V)] * 5,
        out_specs=(any_spec,) * 5,
        scratch_shapes=[dma((5,))],
        compiler_params=pltpu.CompilerParams(vmem_limit_bytes=1024 * 1024),
    )(*outs)
    return outs[0], outs[1], outs[2], outs[3], outs[4].reshape(tile)


def solution(mesh):
    both = ("tm", "space")
    return jax.shard_map(
        per_device,
        mesh=mesh,
        in_specs=(
            P(both, None), P(both, None), P(both, None), P(both, None),
            P("tm", None), P("tm", None), P("tm", None),
            P("tm", None, "space"), P("tm", None, "space"), P("tm", "space", None),
            P("tm", "space"), P(),
        ),
        out_specs=(P(both, None), P(both, None), P(both, None), P(both, None), P(both)),
        check_vma=False,
    )
```

```python
import functools
import math

import jax
import jax.numpy as jnp
from jax import lax
from jax.experimental import pallas as pl
from jax.experimental.pallas import tpu as pltpu
from jax.sharding import PartitionSpec as P

MESH = pl.DeviceIdType.MESH
F32 = jnp.float32
UNROLL = 5
BF16 = jnp.bfloat16

HEAD = 128
REACH = 64
NT = (((1,), (1,)), ((), ()))
TN = (((0,), (0,)), ((), ()))
ORDER = (10, 5, 15, 7, 13, 6, 9, 14, 11, 2, 8, 1, 4, 3, 12)


def kernel(
    clips, aq, ak, av, ao, fq, fo, fk, wg, wu, wd, gf,
    o_q, o_k, o_v, o_f, o_r,
    q_b, o_b, k_b, w_b, wd_b, f_b, aq_b, ao_b, kx, vx,
    gu, g_t, gtot0, gtot1, rx0, rx1, cout0, cout1, cin0, cin1, ip, prx, psum, rsx,
    dk_f, dv_f, dkv_s, dkv_r, f_t, bias, rate_s, rate_r, line,
    ld, halo_s, halo_r, a1_s, a1_r, a2_s, a2_r, pr_s, pr_r, rs_s, rs_r, dk_s, dk_r, rt_s, rt_r,
):
    tm, sp = lax.axis_index("tm"), lax.axis_index("space")
    mz, my = tm // 4, tm % 4
    mx, mk = sp // 2, sp % 2
    rows, hid = gf.shape
    feat = fq.shape[1]
    half = feat // 2
    tile = aq.shape[0]
    parts, starts_at = (2 * hid // 3, hid // 3), (0, 2 * hid // 3)
    gtot, rx, cout, cin = (gtot0, gtot1), (rx0, rx1), (cout0, cout1), (cin0, cin1)
    rt = 256

    barrier = pltpu.get_barrier_semaphore()
    for j in range(1, 16):
        pl.semaphore_signal(barrier, inc=1, device_id={"tm": lax.rem(tm + j, 16)}, device_id_type=MESH)
    for j in range(1, 8):
        pl.semaphore_signal(barrier, inc=1, device_id={"space": lax.rem(sp + j, 8)}, device_id_type=MESH)

    def load(i, src, dst):
        return pltpu.make_async_copy(src, dst, ld.at[i])

    def weights(n):
        mine = pl.ds(starts_at[n], parts[n])
        return [
            load(3 * n, wg.at[0, :, mine], w_b.at[:, pl.ds(2 * starts_at[n], parts[n])]),
            load(3 * n + 1, wu.at[0, :, mine], w_b.at[:, pl.ds(2 * starts_at[n] + parts[n], parts[n])]),
            load(3 * n + 2, wd.at[0, mine], wd_b.at[mine]),
        ]

    def block(r):
        return pl.ds(pl.multiple_of(r * rt, rt), rt)

    def inputs(r):
        return [
            load(6 + r, fq.at[block(r)], q_b.at[block(r)]),
            load(10 + r, fo.at[block(r)], o_b.at[block(r)]),
        ]

    later = [
        load(14, aq, aq_b),
        load(15, ao, ao_b),
        load(16, ak, kx.at[pl.ds(REACH, tile)]),
        load(17, av, vx.at[pl.ds(REACH, tile)]),
        load(18, fk, k_b),
        load(19, gf, f_b),
    ]
    for c in weights(0):
        c.start()
    for r in range(2):
        for c in inputs(r):
            c.start()

    left, right = lax.rem(sp + 7, 8), lax.rem(sp + 1, 8)

    def halo(i, src, dst, to):
        return pltpu.make_async_remote_copy(
            src_ref=src, dst_ref=dst, send_sem=halo_s.at[i], recv_sem=halo_r.at[i],
            device_id={"space": to}, device_id_type=MESH,
        )

    halos = [
        halo(0, ak.at[pl.ds(0, REACH)], kx.at[pl.ds(REACH + tile, REACH)], left),
        halo(1, av.at[pl.ds(0, REACH)], vx.at[pl.ds(REACH + tile, REACH)], left),
        halo(2, ak.at[pl.ds(tile - REACH, REACH)], kx.at[pl.ds(0, REACH)], right),
        halo(3, av.at[pl.ds(tile - REACH, REACH)], vx.at[pl.ds(0, REACH)], right),
    ]

    def peer(kk):
        dz, dy = kk // 4, kk % 4
        return lax.rem(mz + dz, 4) * 4 + lax.rem(my + dy, 4)

    def slice_of(refs, n, d):
        blk = parts[n] // 8
        down, over = pl.multiple_of((d // 2) * blk, 16), pl.multiple_of(lax.rem(d, 2) * half, 128)
        return refs[n].at[pl.ds(down, blk), pl.ds(over, half)]

    def out_copy(n, kk):
        d = peer(kk)
        return pltpu.make_async_remote_copy(
            src_ref=slice_of(gtot, n, d), dst_ref=rx[n].at[tm],
            send_sem=a1_s.at[n * 16 + kk], recv_sem=a1_r.at[n * 16 + kk],
            device_id={"tm": d}, device_id_type=MESH,
        )

    def carry_copy(n, kk):
        d = peer(kk)
        return pltpu.make_async_remote_copy(
            src_ref=cout[n].at[d], dst_ref=slice_of(cin, n, tm),
            send_sem=a2_s.at[n * 16 + kk], recv_sem=a2_r.at[n * 16 + kk],
            device_id={"tm": d}, device_id_type=MESH,
        )

    for n in range(2):
        part, off = parts[n], starts_at[n]
        for c in weights(n):
            c.wait()
        if n == 0:
            for r in range(2, 4):
                for c in inputs(r):
                    c.start()
            for c in weights(1):
                c.start()

        def rows_step(r, _, n=n, part=part, off=off):
            at = block(r)
            if n == 0:
                for c in inputs(r):
                    c.wait()
            pre = jnp.dot(q_b[at, :], w_b[:, pl.ds(2 * off, 2 * part)], preferred_element_type=F32)
            hg = lax.dot_general(o_b[at, :], wd_b[pl.ds(off, part), :], NT, preferred_element_type=F32)
            gate, up = pre[:, :part], pre[:, part:]
            sig = 1.0 / (1.0 + jnp.exp(-gate))
            g = (hg * up * sig * (1.0 + gate * (1.0 - sig))).astype(BF16)
            gu[at, pl.ds(2 * off, part)] = g
            gu[at, pl.ds(2 * off + part, part)] = (hg * (gate * sig)).astype(BF16)
            g_t[pl.ds(off, part), at] = g.T
            return 0

        lax.fori_loop(0, rows // rt, rows_step, 0)
        if n == 0:
            for c in later:
                c.start()

        def total_step(i, _, n=n, part=part, off=off):
            at = pl.ds(pl.multiple_of(i * 256, 256), 256)
            total = jnp.dot(g_t[pl.ds(off, part), :], q_b[:, at], preferred_element_type=F32)
            gtot[n][:, at] = total.astype(BF16)
            return 0

        lax.fori_loop(0, feat // 256, total_step, 0)
        if n == 0:
            pl.semaphore_wait(barrier, 22)
            for c in halos:
                c.start()
        for kk in ORDER:
            out_copy(n, kk).start()
        rx[n][tm] = slice_of(gtot, n, tm)[...]

    s1 = clips[0]
    s2 = s1 + clips[1]
    s3 = s2 + clips[2]

    def carries(n):
        for kk in ORDER:
            out_copy(n, kk).wait_recv()

        def scan_step(i, carry):
            c = 15 - i
            cout[n][c] = carry.astype(BF16)
            starts = (c == 0) | (c == s1) | (c == s2) | (c == s3)
            keep = jnp.where(starts, 0.0, 1.0).astype(F32)
            return keep * (carry + rx[n][c].astype(F32))

        lax.fori_loop(0, 16, scan_step, jnp.zeros((parts[n] // 8, half), F32))
        for kk in ORDER:
            carry_copy(n, kk).start()
        slice_of(cin, n, tm)[...] = cout[n][tm]

    def partner_copy(x):
        return pltpu.make_async_remote_copy(
            src_ref=ip.at[pl.ds(pl.multiple_of(x * 2 * tile + (1 - mk) * tile, tile), tile)], dst_ref=prx.at[x],
            send_sem=pr_s.at[x], recv_sem=pr_r.at[x],
            device_id={"space": mx * 2 + 1 - mk}, device_id_type=MESH,
        )

    def input_step(i, _):
        x = lax.rem(mx + 2 + i, 4)
        at = pl.ds(pl.multiple_of(x * rt, rt), rt)
        terms = lax.dot_general(gu[at, :], w_b[...], NT, preferred_element_type=F32)
        ip[at, :] = terms.astype(BF16)
        partner_copy(x).start()
        return 0

    lax.fori_loop(0, 4, input_step, 0)

    ahead, behind = 1 + 2 * mk, 3 - 2 * mk

    def rs_copy(i, to):
        return pltpu.make_async_remote_copy(
            src_ref=psum.at[i], dst_ref=rsx.at[i], send_sem=rs_s.at[i], recv_sem=rs_r.at[i],
            device_id={"space": lax.rem(mx + to, 4) * 2 + mk}, device_id_type=MESH,
        )

    relay = [rs_copy(0, ahead), rs_copy(1, ahead), rs_copy(2, behind)]

    def pair_sum(to):
        x = lax.rem(mx + to, 4)
        partner_copy(x).wait_recv()
        mine = ip[pl.ds(pl.multiple_of(x * 2 * tile + mk * tile, tile), tile), :]
        return mine.astype(F32) + prx[x].astype(F32)

    psum[0] = pair_sum(2).astype(BF16)
    relay[0].start()
    psum[2] = pair_sum(behind).astype(BF16)
    relay[2].start()

    for c in later[:4]:
        c.wait()
    for c in halos:
        c.wait()
    key = lax.broadcasted_iota(jnp.int32, (2 * tile, tile), 0)
    query = lax.broadcasted_iota(jnp.int32, (2 * tile, tile), 1)
    apart = key - query
    place = key + (sp * tile - REACH)
    allowed = (apart >= 0) & (apart <= 2 * REACH) & (place >= 0) & (place < rows)
    bias[...] = jnp.where(allowed, 0.0, -1e30)
    scaling = 1.0 / math.sqrt(HEAD)

    def one_head(hh):
        at = pl.ds(pl.multiple_of(hh * HEAD, HEAD), HEAD)
        q, g, k, v = aq_b[:, at], ao_b[:, at], kx[:, at], vx[:, at]
        s = lax.dot_general(k, q, NT, preferred_element_type=F32) * (scaling * math.log2(math.e)) + bias[...]
        e = jnp.exp2(s - jnp.max(s, axis=0, keepdims=True))
        p = e * (1.0 / jnp.sum(e, axis=0, keepdims=True))
        pb = p.astype(BF16)
        dp = lax.dot_general(v, g, NT, preferred_element_type=F32)
        delta = jnp.sum(pb.astype(F32) * dp, axis=0, keepdims=True)
        ds = (p * (dp - delta)).astype(BF16)
        dv = jnp.dot(pb, g, preferred_element_type=F32)
        dk = jnp.dot(ds, q, preferred_element_type=F32) * scaling
        o_q[:, at] = (lax.dot_general(ds, k, TN, preferred_element_type=F32) * scaling).astype(BF16)
        dk_f[:, at] = dk[REACH : REACH + tile]
        dv_f[:, at] = dv[REACH : REACH + tile]
        dkv_s[0, 0, :, at] = dk[:REACH].astype(BF16)
        dkv_s[0, 1, :, at] = dv[:REACH].astype(BF16)
        dkv_s[1, 0, :, at] = dk[REACH + tile :].astype(BF16)
        dkv_s[1, 1, :, at] = dv[REACH + tile :].astype(BF16)

    def head_step(i, _):
        for j in range(UNROLL):
            one_head(i * UNROLL + j)
        return 0

    steps = aq.shape[1] // HEAD // UNROLL
    lax.fori_loop(0, steps // 2, head_step, 0)
    carries(0)
    lax.fori_loop(steps // 2, steps, head_step, 0)

    def back(i, to):
        return pltpu.make_async_remote_copy(
            src_ref=dkv_s.at[i], dst_ref=dkv_r.at[i], send_sem=dk_s.at[i], recv_sem=dk_r.at[i],
            device_id={"space": to}, device_id_type=MESH,
        )

    backs = [back(0, left), back(1, right)]
    for c in backs:
        c.start()

    for c in later[4:]:
        c.wait()

    def turn_step(r, _):
        at = pl.ds(pl.multiple_of(r * rt, rt), rt)
        f_t[:, at] = f_b[at, :].T
        return 0

    lax.fori_loop(0, rows // rt, turn_step, 0)

    carries(1)
    relay[0].wait_recv()
    psum[1] = (pair_sum(ahead) + rsx[0].astype(F32)).astype(BF16)
    relay[1].start()

    def rate_copy(d):
        j = lax.rem(d - sp + 8, 8)
        return pltpu.make_async_remote_copy(
            src_ref=rate_s.at[d], dst_ref=rate_r.at[j], send_sem=rt_s.at[j], recv_sem=rt_r.at[j],
            device_id={"space": d}, device_id_type=MESH,
        )

    def rate_part(n, r):
        at = block(r)
        kc = lax.dot_general(cin[n][...], k_b[at, :], NT, preferred_element_type=F32)
        factors = f_t[pl.ds(starts_at[n], parts[n]), at].astype(F32)
        return jnp.sum(kc * factors, axis=0, keepdims=True)

    def rate_first(r, _):
        line[r] = rate_part(0, r)
        return 0

    def rate_second(r):
        whole = (line[r] + rate_part(1, r)) * (1.0 / rows)
        rate_s[2 * r] = jnp.broadcast_to(whole[:, :tile], (8, tile))
        rate_s[2 * r + 1] = jnp.broadcast_to(whole[:, tile:], (8, tile))

    for kk in ORDER:
        carry_copy(0, kk).wait_recv()
    lax.fori_loop(0, rows // rt, rate_first, 0)

    total = pair_sum(0)
    for i in (2, 1):
        relay[i].wait_recv()
        total = total + rsx[i].astype(F32)
    o_f[...] = total.astype(BF16)

    for c in backs:
        c.wait_recv()
    o_k[pl.ds(0, REACH), :] = (dk_f[pl.ds(0, REACH), :] + dkv_r[1, 0].astype(F32)).astype(BF16)
    o_k[pl.ds(tile - REACH, REACH), :] = (dk_f[pl.ds(tile - REACH, REACH), :] + dkv_r[0, 0].astype(F32)).astype(BF16)
    o_v[pl.ds(0, REACH), :] = (dv_f[pl.ds(0, REACH), :] + dkv_r[1, 1].astype(F32)).astype(BF16)
    o_v[pl.ds(tile - REACH, REACH), :] = (dv_f[pl.ds(tile - REACH, REACH), :] + dkv_r[0, 1].astype(F32)).astype(BF16)

    for kk in ORDER:
        carry_copy(1, kk).wait_recv()

    def rate_away(i):
        r = lax.rem(mx + 2 + i, 4)
        rate_second(r)
        rate_copy(2 * r).start()
        rate_copy(2 * r + 1).start()

    for i in (0, 1, 3):
        rate_away(i)
    rate_second(mx)
    rate_copy(2 * mx + 1 - mk).start()
    rate = rate_s[sp]
    for j in range(1, 8):
        rate_copy(lax.rem(sp + j, 8)).wait_recv()
        rate = rate + rate_r[j]
    o_r[...] = rate[0:1, :]

    for kk in ORDER:
        for n in range(2):
            out_copy(n, kk).wait_send()
            carry_copy(n, kk).wait_send()
    for x in range(4):
        partner_copy(x).wait_send()
    for c in relay:
        c.wait_send()
    for c in backs:
        c.wait_send()
    for j in range(1, 8):
        rate_copy(lax.rem(sp + j, 8)).wait_send()


def put_out(a, b, c, d, e, oa, ob, oc, od, oe, sem):
    copies = [pltpu.make_async_copy(src, dst, sem.at[i])
              for i, (src, dst) in enumerate(((a, oa), (b, ob), (c, oc), (d, od), (e, oe)))]
    for c in copies:
        c.start()
    for c in copies:
        c.wait()


def per_device(attn_query, attn_key, attn_value, attn_outgrad, fast_query, fast_outgrad, fast_key,
               gate_weights, up_weights, down_weights, gate_factor, clip_groups):
    tile, width = attn_query.shape
    rows, hid = gate_factor.shape
    feat = fast_query.shape[1]
    half, third = feat // 2, hid // 3
    blk = third // 8
    any_spec = pl.BlockSpec(memory_space=pl.ANY)
    dma = pltpu.SemaphoreType.DMA
    V = pltpu.VMEM
    outs = pl.pallas_call(
        kernel,
        out_shape=(
            V((tile, width), BF16), V((tile, width), BF16), V((tile, width), BF16),
            V((tile, feat), BF16), V((1, tile), F32),
        ),
        in_specs=[pl.BlockSpec(memory_space=pltpu.SMEM)] + [any_spec] * 11,
        out_specs=(pl.BlockSpec(memory_space=V),) * 5,
        scratch_shapes=[
            V((rows, feat), BF16), V((rows, feat), BF16), V((rows, feat), BF16),
            V((feat, 2 * hid), BF16), V((hid, feat), BF16), V((rows, hid), BF16),
            V((tile, width), BF16), V((tile, width), BF16), V((2 * tile, width), BF16), V((2 * tile, width), BF16),
            V((rows, 2 * hid), BF16), V((hid, rows), BF16), V((2 * third, feat), BF16), V((third, feat), BF16),
            V((16, 2 * blk, half), BF16), V((16, blk, half), BF16), V((16, 2 * blk, half), BF16), V((16, blk, half), BF16),
            V((2 * third, feat), BF16), V((third, feat), BF16),
            V((rows, feat), BF16), V((4, tile, feat), BF16), V((3, tile, feat), BF16), V((3, tile, feat), BF16),
            V((tile, width), F32), V((tile, width), F32),
            V((2, 2, REACH, width), BF16), V((2, 2, REACH, width), BF16),
            V((hid, rows), BF16), V((2 * tile, tile), F32),
            V((8, 8, tile), F32), V((8, 8, tile), F32), V((4, 1, 256), F32),
            dma((20,)), dma((4,)), dma((4,)), dma((32,)), dma((32,)), dma((32,)), dma((32,)),
            dma((4,)), dma((4,)), dma((3,)), dma((3,)), dma((2,)), dma((2,)), dma((8,)), dma((8,)),
        ],
        compiler_params=pltpu.CompilerParams(
            collective_id=0, has_side_effects=True, vmem_limit_bytes=64_500_000
        ),
    )(clip_groups, attn_query, attn_key, attn_value, attn_outgrad, fast_query, fast_outgrad, fast_key,
      gate_weights, up_weights, down_weights, gate_factor)
    outs = pl.pallas_call(
        put_out,
        out_shape=tuple(jax.ShapeDtypeStruct(o.shape, o.dtype) for o in outs),
        in_specs=[pl.BlockSpec(memory_space=V)] * 5,
        out_specs=(any_spec,) * 5,
        scratch_shapes=[dma((5,))],
        compiler_params=pltpu.CompilerParams(vmem_limit_bytes=1024 * 1024),
    )(*outs)
    return outs[0], outs[1], outs[2], outs[3], outs[4].reshape(tile)


def solution(mesh):
    both = ("tm", "space")
    return jax.shard_map(
        per_device,
        mesh=mesh,
        in_specs=(
            P(both, None), P(both, None), P(both, None), P(both, None),
            P("tm", None), P("tm", None), P("tm", None),
            P("tm", None, "space"), P("tm", None, "space"), P("tm", "space", None),
            P("tm", "space"), P(),
        ),
        out_specs=(P(both, None), P(both, None), P(both, None), P(both, None), P(both)),
        check_vma=False,
    )
```

```python
import functools
import math

import jax
import jax.numpy as jnp
from jax import lax
from jax.experimental import pallas as pl
from jax.experimental.pallas import tpu as pltpu
from jax.sharding import PartitionSpec as P

MESH = pl.DeviceIdType.MESH
F32 = jnp.float32
UNROLL = 10
BF16 = jnp.bfloat16

HEAD = 128
REACH = 64
NT = (((1,), (1,)), ((), ()))
TN = (((0,), (0,)), ((), ()))
ORDER = (10, 5, 15, 7, 13, 6, 9, 14, 11, 2, 8, 1, 4, 3, 12)


def kernel(
    clips, aq, ak, av, ao, fq, fo, fk, wg, wu, wd, gf,
    o_q, o_k, o_v, o_f, o_r,
    q_b, o_b, k_b, w_b, wd_b, f_b, aq_b, ao_b, kx, vx,
    gu, g_t, gtot0, gtot1, rx0, rx1, cout0, cout1, cin0, cin1, ip, prx, psum, rsx,
    dk_f, dv_f, dkv_s, dkv_r, f_t, bias, rate_s, rate_r, line,
    ld, halo_s, halo_r, a1_s, a1_r, a2_s, a2_r, pr_s, pr_r, rs_s, rs_r, dk_s, dk_r, rt_s, rt_r,
):
    tm, sp = lax.axis_index("tm"), lax.axis_index("space")
    mz, my = tm // 4, tm % 4
    mx, mk = sp // 2, sp % 2
    rows, hid = gf.shape
    feat = fq.shape[1]
    half = feat // 2
    tile = aq.shape[0]
    parts, starts_at = (2 * hid // 3, hid // 3), (0, 2 * hid // 3)
    gtot, rx, cout, cin = (gtot0, gtot1), (rx0, rx1), (cout0, cout1), (cin0, cin1)
    rt = 256

    barrier = pltpu.get_barrier_semaphore()
    for j in range(1, 16):
        pl.semaphore_signal(barrier, inc=1, device_id={"tm": lax.rem(tm + j, 16)}, device_id_type=MESH)
    for j in range(1, 8):
        pl.semaphore_signal(barrier, inc=1, device_id={"space": lax.rem(sp + j, 8)}, device_id_type=MESH)

    def load(i, src, dst):
        return pltpu.make_async_copy(src, dst, ld.at[i])

    def weights(n):
        mine = pl.ds(starts_at[n], parts[n])
        return [
            load(3 * n, wg.at[0, :, mine], w_b.at[:, pl.ds(2 * starts_at[n], parts[n])]),
            load(3 * n + 1, wu.at[0, :, mine], w_b.at[:, pl.ds(2 * starts_at[n] + parts[n], parts[n])]),
            load(3 * n + 2, wd.at[0, mine], wd_b.at[mine]),
        ]

    def block(r):
        return pl.ds(pl.multiple_of(r * rt, rt), rt)

    def inputs(r):
        return [
            load(6 + r, fq.at[block(r)], q_b.at[block(r)]),
            load(10 + r, fo.at[block(r)], o_b.at[block(r)]),
        ]

    later = [
        load(14, aq, aq_b),
        load(15, ao, ao_b),
        load(16, ak, kx.at[pl.ds(REACH, tile)]),
        load(17, av, vx.at[pl.ds(REACH, tile)]),
        load(18, fk, k_b),
        load(19, gf, f_b),
    ]
    for c in weights(0):
        c.start()
    for r in range(2):
        for c in inputs(r):
            c.start()

    left, right = lax.rem(sp + 7, 8), lax.rem(sp + 1, 8)

    def halo(i, src, dst, to):
        return pltpu.make_async_remote_copy(
            src_ref=src, dst_ref=dst, send_sem=halo_s.at[i], recv_sem=halo_r.at[i],
            device_id={"space": to}, device_id_type=MESH,
        )

    halos = [
        halo(0, ak.at[pl.ds(0, REACH)], kx.at[pl.ds(REACH + tile, REACH)], left),
        halo(1, av.at[pl.ds(0, REACH)], vx.at[pl.ds(REACH + tile, REACH)], left),
        halo(2, ak.at[pl.ds(tile - REACH, REACH)], kx.at[pl.ds(0, REACH)], right),
        halo(3, av.at[pl.ds(tile - REACH, REACH)], vx.at[pl.ds(0, REACH)], right),
    ]

    def peer(kk):
        dz, dy = kk // 4, kk % 4
        return lax.rem(mz + dz, 4) * 4 + lax.rem(my + dy, 4)

    def slice_of(refs, n, d):
        blk = parts[n] // 8
        down, over = pl.multiple_of((d // 2) * blk, 16), pl.multiple_of(lax.rem(d, 2) * half, 128)
        return refs[n].at[pl.ds(down, blk), pl.ds(over, half)]

    def out_copy(n, kk):
        d = peer(kk)
        return pltpu.make_async_remote_copy(
            src_ref=slice_of(gtot, n, d), dst_ref=rx[n].at[tm],
            send_sem=a1_s.at[n * 16 + kk], recv_sem=a1_r.at[n * 16 + kk],
            device_id={"tm": d}, device_id_type=MESH,
        )

    def carry_copy(n, kk):
        d = peer(kk)
        return pltpu.make_async_remote_copy(
            src_ref=cout[n].at[d], dst_ref=slice_of(cin, n, tm),
            send_sem=a2_s.at[n * 16 + kk], recv_sem=a2_r.at[n * 16 + kk],
            device_id={"tm": d}, device_id_type=MESH,
        )

    for n in range(2):
        part, off = parts[n], starts_at[n]
        for c in weights(n):
            c.wait()
        if n == 0:
            for r in range(2, 4):
                for c in inputs(r):
                    c.start()
            for c in weights(1):
                c.start()

        def rows_step(r, _, n=n, part=part, off=off):
            at = block(r)
            if n == 0:
                for c in inputs(r):
                    c.wait()
            pre = jnp.dot(q_b[at, :], w_b[:, pl.ds(2 * off, 2 * part)], preferred_element_type=F32)
            hg = lax.dot_general(o_b[at, :], wd_b[pl.ds(off, part), :], NT, preferred_element_type=F32)
            gate, up = pre[:, :part], pre[:, part:]
            sig = 1.0 / (1.0 + jnp.exp(-gate))
            g = (hg * up * sig * (1.0 + gate * (1.0 - sig))).astype(BF16)
            gu[at, pl.ds(2 * off, part)] = g
            gu[at, pl.ds(2 * off + part, part)] = (hg * (gate * sig)).astype(BF16)
            g_t[pl.ds(off, part), at] = g.T
            return 0

        lax.fori_loop(0, rows // rt, rows_step, 0)
        if n == 0:
            for c in later:
                c.start()

        def total_step(i, _, n=n, part=part, off=off):
            at = pl.ds(pl.multiple_of(i * 256, 256), 256)
            total = jnp.dot(g_t[pl.ds(off, part), :], q_b[:, at], preferred_element_type=F32)
            gtot[n][:, at] = total.astype(BF16)
            return 0

        lax.fori_loop(0, feat // 256, total_step, 0)
        if n == 0:
            pl.semaphore_wait(barrier, 22)
            for c in halos:
                c.start()
        for kk in ORDER:
            out_copy(n, kk).start()
        rx[n][tm] = slice_of(gtot, n, tm)[...]

    s1 = clips[0]
    s2 = s1 + clips[1]
    s3 = s2 + clips[2]

    def carries(n):
        for kk in ORDER:
            out_copy(n, kk).wait_recv()

        def scan_step(i, carry):
            c = 15 - i
            cout[n][c] = carry.astype(BF16)
            starts = (c == 0) | (c == s1) | (c == s2) | (c == s3)
            keep = jnp.where(starts, 0.0, 1.0).astype(F32)
            return keep * (carry + rx[n][c].astype(F32))

        lax.fori_loop(0, 16, scan_step, jnp.zeros((parts[n] // 8, half), F32))
        for kk in ORDER:
            carry_copy(n, kk).start()
        slice_of(cin, n, tm)[...] = cout[n][tm]

    def partner_copy(x):
        return pltpu.make_async_remote_copy(
            src_ref=ip.at[pl.ds(pl.multiple_of(x * 2 * tile + (1 - mk) * tile, tile), tile)], dst_ref=prx.at[x],
            send_sem=pr_s.at[x], recv_sem=pr_r.at[x],
            device_id={"space": mx * 2 + 1 - mk}, device_id_type=MESH,
        )

    def input_step(i, _):
        x = lax.rem(mx + 2 + i, 4)
        at = pl.ds(pl.multiple_of(x * rt, rt), rt)
        terms = lax.dot_general(gu[at, :], w_b[...], NT, preferred_element_type=F32)
        ip[at, :] = terms.astype(BF16)
        partner_copy(x).start()
        return 0

    lax.fori_loop(0, 4, input_step, 0)

    ahead, behind = 1 + 2 * mk, 3 - 2 * mk

    def rs_copy(i, to):
        return pltpu.make_async_remote_copy(
            src_ref=psum.at[i], dst_ref=rsx.at[i], send_sem=rs_s.at[i], recv_sem=rs_r.at[i],
            device_id={"space": lax.rem(mx + to, 4) * 2 + mk}, device_id_type=MESH,
        )

    relay = [rs_copy(0, ahead), rs_copy(1, ahead), rs_copy(2, behind)]

    def pair_sum(to):
        x = lax.rem(mx + to, 4)
        partner_copy(x).wait_recv()
        mine = ip[pl.ds(pl.multiple_of(x * 2 * tile + mk * tile, tile), tile), :]
        return mine.astype(F32) + prx[x].astype(F32)

    psum[0] = pair_sum(2).astype(BF16)
    relay[0].start()
    psum[2] = pair_sum(behind).astype(BF16)
    relay[2].start()

    for c in later[:4]:
        c.wait()
    for c in halos:
        c.wait()
    key = lax.broadcasted_iota(jnp.int32, (2 * tile, tile), 0)
    query = lax.broadcasted_iota(jnp.int32, (2 * tile, tile), 1)
    apart = key - query
    place = key + (sp * tile - REACH)
    allowed = (apart >= 0) & (apart <= 2 * REACH) & (place >= 0) & (place < rows)
    bias[...] = jnp.where(allowed, 0.0, -1e30)
    scaling = 1.0 / math.sqrt(HEAD)

    def one_head(hh):
        at = pl.ds(pl.multiple_of(hh * HEAD, HEAD), HEAD)
        q, g, k, v = aq_b[:, at], ao_b[:, at], kx[:, at], vx[:, at]
        s = lax.dot_general(k, q, NT, preferred_element_type=F32) * (scaling * math.log2(math.e)) + bias[...]
        e = jnp.exp2(s - jnp.max(s, axis=0, keepdims=True))
        p = e * (1.0 / jnp.sum(e, axis=0, keepdims=True))
        pb = p.astype(BF16)
        dp = lax.dot_general(v, g, NT, preferred_element_type=F32)
        delta = jnp.sum(pb.astype(F32) * dp, axis=0, keepdims=True)
        ds = (p * (dp - delta)).astype(BF16)
        dv = jnp.dot(pb, g, preferred_element_type=F32)
        dk = jnp.dot(ds, q, preferred_element_type=F32) * scaling
        o_q[:, at] = (lax.dot_general(ds, k, TN, preferred_element_type=F32) * scaling).astype(BF16)
        dk_f[:, at] = dk[REACH : REACH + tile]
        dv_f[:, at] = dv[REACH : REACH + tile]
        dkv_s[0, 0, :, at] = dk[:REACH].astype(BF16)
        dkv_s[0, 1, :, at] = dv[:REACH].astype(BF16)
        dkv_s[1, 0, :, at] = dk[REACH + tile :].astype(BF16)
        dkv_s[1, 1, :, at] = dv[REACH + tile :].astype(BF16)

    def head_step(i, _):
        for j in range(UNROLL):
            one_head(i * UNROLL + j)
        return 0

    steps = aq.shape[1] // HEAD // UNROLL
    lax.fori_loop(0, steps // 2, head_step, 0)
    carries(0)
    lax.fori_loop(steps // 2, steps, head_step, 0)

    def back(i, to):
        return pltpu.make_async_remote_copy(
            src_ref=dkv_s.at[i], dst_ref=dkv_r.at[i], send_sem=dk_s.at[i], recv_sem=dk_r.at[i],
            device_id={"space": to}, device_id_type=MESH,
        )

    backs = [back(0, left), back(1, right)]
    for c in backs:
        c.start()

    for c in later[4:]:
        c.wait()

    def turn_step(r, _):
        at = pl.ds(pl.multiple_of(r * rt, rt), rt)
        f_t[:, at] = f_b[at, :].T
        return 0

    lax.fori_loop(0, rows // rt, turn_step, 0)

    carries(1)
    relay[0].wait_recv()
    psum[1] = (pair_sum(ahead) + rsx[0].astype(F32)).astype(BF16)
    relay[1].start()

    def rate_copy(d):
        j = lax.rem(d - sp + 8, 8)
        return pltpu.make_async_remote_copy(
            src_ref=rate_s.at[d], dst_ref=rate_r.at[j], send_sem=rt_s.at[j], recv_sem=rt_r.at[j],
            device_id={"space": d}, device_id_type=MESH,
        )

    def rate_part(n, r):
        at = block(r)
        kc = lax.dot_general(cin[n][...], k_b[at, :], NT, preferred_element_type=F32)
        factors = f_t[pl.ds(starts_at[n], parts[n]), at].astype(F32)
        return jnp.sum(kc * factors, axis=0, keepdims=True)

    def rate_first(r, _):
        line[r] = rate_part(0, r)
        return 0

    def rate_second(r):
        whole = (line[r] + rate_part(1, r)) * (1.0 / rows)
        rate_s[2 * r] = jnp.broadcast_to(whole[:, :tile], (8, tile))
        rate_s[2 * r + 1] = jnp.broadcast_to(whole[:, tile:], (8, tile))

    for kk in ORDER:
        carry_copy(0, kk).wait_recv()
    lax.fori_loop(0, rows // rt, rate_first, 0)

    total = pair_sum(0)
    for i in (2, 1):
        relay[i].wait_recv()
        total = total + rsx[i].astype(F32)
    o_f[...] = total.astype(BF16)

    for c in backs:
        c.wait_recv()
    o_k[pl.ds(0, REACH), :] = (dk_f[pl.ds(0, REACH), :] + dkv_r[1, 0].astype(F32)).astype(BF16)
    o_k[pl.ds(tile - REACH, REACH), :] = (dk_f[pl.ds(tile - REACH, REACH), :] + dkv_r[0, 0].astype(F32)).astype(BF16)
    o_v[pl.ds(0, REACH), :] = (dv_f[pl.ds(0, REACH), :] + dkv_r[1, 1].astype(F32)).astype(BF16)
    o_v[pl.ds(tile - REACH, REACH), :] = (dv_f[pl.ds(tile - REACH, REACH), :] + dkv_r[0, 1].astype(F32)).astype(BF16)

    for kk in ORDER:
        carry_copy(1, kk).wait_recv()

    def rate_away(i):
        r = lax.rem(mx + 2 + i, 4)
        rate_second(r)
        rate_copy(2 * r).start()
        rate_copy(2 * r + 1).start()

    for i in (0, 1, 3):
        rate_away(i)
    rate_second(mx)
    rate_copy(2 * mx + 1 - mk).start()
    rate = rate_s[sp]
    for j in range(1, 8):
        rate_copy(lax.rem(sp + j, 8)).wait_recv()
        rate = rate + rate_r[j]
    o_r[...] = rate[0:1, :]

    for kk in ORDER:
        for n in range(2):
            out_copy(n, kk).wait_send()
            carry_copy(n, kk).wait_send()
    for x in range(4):
        partner_copy(x).wait_send()
    for c in relay:
        c.wait_send()
    for c in backs:
        c.wait_send()
    for j in range(1, 8):
        rate_copy(lax.rem(sp + j, 8)).wait_send()


def put_out(a, b, c, d, e, oa, ob, oc, od, oe, sem):
    pairs = [(d, od), (e, oe)]
    for src, dst in ((a, oa), (b, ob), (c, oc)):
        rows = src.shape[0] // 4
        pairs += [(src.at[pl.ds(i * rows, rows)], dst.at[pl.ds(i * rows, rows)]) for i in range(4)]
    copies = [pltpu.make_async_copy(src, dst, sem.at[i]) for i, (src, dst) in enumerate(pairs)]
    for c in copies:
        c.start()
    for c in copies:
        c.wait()


def per_device(attn_query, attn_key, attn_value, attn_outgrad, fast_query, fast_outgrad, fast_key,
               gate_weights, up_weights, down_weights, gate_factor, clip_groups):
    tile, width = attn_query.shape
    rows, hid = gate_factor.shape
    feat = fast_query.shape[1]
    half, third = feat // 2, hid // 3
    blk = third // 8
    any_spec = pl.BlockSpec(memory_space=pl.ANY)
    dma = pltpu.SemaphoreType.DMA
    V = pltpu.VMEM
    outs = pl.pallas_call(
        kernel,
        out_shape=(
            V((tile, width), BF16), V((tile, width), BF16), V((tile, width), BF16),
            V((tile, feat), BF16), V((1, tile), F32),
        ),
        in_specs=[pl.BlockSpec(memory_space=pltpu.SMEM)] + [any_spec] * 11,
        out_specs=(pl.BlockSpec(memory_space=V),) * 5,
        scratch_shapes=[
            V((rows, feat), BF16), V((rows, feat), BF16), V((rows, feat), BF16),
            V((feat, 2 * hid), BF16), V((hid, feat), BF16), V((rows, hid), BF16),
            V((tile, width), BF16), V((tile, width), BF16), V((2 * tile, width), BF16), V((2 * tile, width), BF16),
            V((rows, 2 * hid), BF16), V((hid, rows), BF16), V((2 * third, feat), BF16), V((third, feat), BF16),
            V((16, 2 * blk, half), BF16), V((16, blk, half), BF16), V((16, 2 * blk, half), BF16), V((16, blk, half), BF16),
            V((2 * third, feat), BF16), V((third, feat), BF16),
            V((rows, feat), BF16), V((4, tile, feat), BF16), V((3, tile, feat), BF16), V((3, tile, feat), BF16),
            V((tile, width), F32), V((tile, width), F32),
            V((2, 2, REACH, width), BF16), V((2, 2, REACH, width), BF16),
            V((hid, rows), BF16), V((2 * tile, tile), F32),
            V((8, 8, tile), F32), V((8, 8, tile), F32), V((4, 1, 256), F32),
            dma((20,)), dma((4,)), dma((4,)), dma((32,)), dma((32,)), dma((32,)), dma((32,)),
            dma((4,)), dma((4,)), dma((3,)), dma((3,)), dma((2,)), dma((2,)), dma((8,)), dma((8,)),
        ],
        compiler_params=pltpu.CompilerParams(
            collective_id=0, has_side_effects=True, vmem_limit_bytes=64_500_000
        ),
    )(clip_groups, attn_query, attn_key, attn_value, attn_outgrad, fast_query, fast_outgrad, fast_key,
      gate_weights, up_weights, down_weights, gate_factor)
    outs = pl.pallas_call(
        put_out,
        out_shape=tuple(jax.ShapeDtypeStruct(o.shape, o.dtype) for o in outs),
        in_specs=[pl.BlockSpec(memory_space=V)] * 5,
        out_specs=(any_spec,) * 5,
        scratch_shapes=[dma((14,))],
        compiler_params=pltpu.CompilerParams(vmem_limit_bytes=1024 * 1024),
    )(*outs)
    return outs[0], outs[1], outs[2], outs[3], outs[4].reshape(tile)


def solution(mesh):
    both = ("tm", "space")
    return jax.shard_map(
        per_device,
        mesh=mesh,
        in_specs=(
            P(both, None), P(both, None), P(both, None), P(both, None),
            P("tm", None), P("tm", None), P("tm", None),
            P("tm", None, "space"), P("tm", None, "space"), P("tm", "space", None),
            P("tm", "space"), P(),
        ),
        out_specs=(P(both, None), P(both, None), P(both, None), P(both, None), P(both)),
        check_vma=False,
    )
```
